512 devices in a mesh: lat: 128 (over y, z, x_hi), lon: 4 (over x_lo, core).
Axes of the slice: x: 4 (x_hi: 2, x_lo: 2; x = x_hi * 2 + x_lo), y: 4, z: 16, core: 2. Of those that a mesh axis runs over, the one named last changes fastest.
Arguments:
- grid_state: bfloat16 [256, 720, 640], P('lat', 'lon'), may hold values from -6 to 6
- conv_weight: float32 [3, 3, 640], replicated, may hold values from -2.4 to 2.4
- spectral_gain: float32 [2, 256, 640], P(None, None, 'lon'), may hold values from -4 to 4
- spectral_weight: bfloat16 [2, 640, 640], P(None, None, 'lon'), may hold values from -0.125 to 0.125
- norm_gain: float32 [640], replicated, may hold values from 0.1 to 1.9
- expand_weight: bfloat16 [640, 1280], replicated, may hold values from -0.25 to 0.25
- reduce_weight: bfloat16 [1280, 640], replicated, may hold values from -0.15625 to 0.15625
Outputs:
- block_output: bfloat16 [256, 720, 640], P('lat', 'lon')
The draws below stay inside these ranges and needn't reach their ends.
All inputs are finite; a program needn't handle non-finite values.
Results may differ from the reference program's by a relative error of at most 0.015.
Values may be sent and summed in bfloat16 or wider, within the bound.
A program may use at most 64 MiB of HBM per device.

```python
import math
import jax
import jax.numpy as jnp
from jax import lax

C = 640
FFN = 1280
M = 256
NLON = 720
NLAT = 256


def levels(key, dims, split, low, largest):
    loudness = 1.0
    for position, blocks in split:
        draws = jax.random.uniform(jax.random.fold_in(jax.random.fold_in(key, 6), position), (blocks,), jnp.float32, low / len(split), largest / len(split))
        loudness = loudness * jnp.repeat(jnp.exp(draws), dims[position] // blocks).reshape((-1,) + (1,) * (len(dims) - 1 - position))
    return loudness


def normal_values(own_key, extent, spread, limit, pieces=(), kind=jnp.bfloat16):
    values = spread * jax.random.normal(own_key, extent, jnp.float32)
    if pieces:
        values = values * levels(own_key, extent, pieces, -0.22, 0.18)
    return jnp.clip(values, -limit, limit).astype(kind)


def setup_inputs(seed: int = 0) -> dict:
    key_of = jax.random.split(jax.random.key(seed), 8)
    return {
        "grid_state": normal_values(key_of[0], (NLAT, NLON, C), 1.0, 6.0, ((0, 128), (1, 4))),
        "conv_weight": normal_values(key_of[1], (3, 3, C), 0.4, 2.4, (), jnp.float32),
        "spectral_gain": normal_values(key_of[2], (2, M, C), 1.0, 4.0, ((2, 4),), jnp.float32),
        "spectral_weight": normal_values(key_of[3], (2, C, C), (4 * C) ** -0.5, 0.125, ((2, 4),)),
        "norm_gain": jnp.clip(1.0 + 0.18 * jax.random.normal(key_of[4], (C,), jnp.float32), 0.1, 1.9),
        "expand_weight": normal_values(key_of[5], (C, FFN), C ** -0.5, 0.25),
        "reduce_weight": normal_values(key_of[6], (FFN, C), FFN ** -0.5, 0.15625),
    }


norm_eps = 1e-06
underflow_cut = -60.0

def legendre_table(orders, lat_total, degree_count):
    colatitude = (jnp.arange(lat_total, dtype=jnp.float32) + 0.5) * (math.pi / lat_total)
    cosines = jnp.cos(colatitude)
    sine_values = jnp.sin(colatitude)
    rank_values = jnp.arange(1, degree_count + 1, dtype=jnp.int32)
    rank_float = rank_values.astype(jnp.float32)
    log_terms = 0.5 * jnp.log((2.0 * rank_float + 1.0) / (2.0 * rank_float))
    log_norm = lax.optimization_barrier(jnp.sum(jnp.where(rank_values[None, :] <= orders[:, None], log_terms[None, :], jnp.float32(0.0)), axis=1))
    order_float = orders.astype(jnp.float32)[:, None]
    log_start = -0.5 * math.log(4.0 * math.pi) + log_norm[:, None] + order_float * jnp.log(sine_values)[None, :]
    start_value = jnp.where(log_start > underflow_cut, jnp.exp(jnp.maximum(log_start, underflow_cut)), jnp.float32(0.0))

    def advance(totals, degree):
        previous, earlier = totals
        degree_float = degree.astype(jnp.float32)
        raise_coef = jnp.sqrt(jnp.maximum(4.0 * degree_float * degree_float - 1.0, 0.0) / jnp.maximum(degree_float * degree_float - order_float * order_float, 1.0))
        lower_coef = jnp.sqrt(jnp.maximum((degree_float - 1.0) ** 2 - order_float * order_float, 0.0) / jnp.maximum(4.0 * (degree_float - 1.0) ** 2 - 1.0, 1.0))
        recurred = raise_coef * (cosines[None, :] * previous - lower_coef * earlier)
        current = jnp.where(degree < orders[:, None], jnp.float32(0.0), jnp.where(degree == orders[:, None], start_value, recurred))
        return ((current, previous), current)
    blank = jnp.zeros((orders.shape[0], lat_total), jnp.float32)
    unused, table_values = lax.scan(advance, (blank, blank), jnp.arange(degree_count, dtype=jnp.int32))
    return table_values

def quadrature(lat_total):
    colatitude = (jnp.arange(lat_total, dtype=jnp.float32) + 0.5) * (math.pi / lat_total)
    return 2.0 * math.pi * math.pi / lat_total * jnp.sin(colatitude)

def fourier_table(longitudes, lon_total, mode_count):
    mode_index = jnp.arange(mode_count, dtype=jnp.int32)
    phase_index = longitudes[:, None] * mode_index[None, :] % lon_total
    angles = phase_index.astype(jnp.float32) * (2.0 * math.pi / lon_total)
    return (jnp.stack([jnp.cos(angles), -jnp.sin(angles)], axis=1) / lon_total).astype(jnp.bfloat16)

def synthesis_table(longitudes, lon_total, mode_count):
    mode_index = jnp.arange(mode_count, dtype=jnp.int32)
    phase_index = mode_index[:, None] * longitudes[None, :] % lon_total
    angles = phase_index.astype(jnp.float32) * (2.0 * math.pi / lon_total)
    doubling = jnp.where(mode_index == 0, 1.0, 2.0).astype(jnp.float32)[:, None]
    return jnp.stack([doubling * jnp.cos(angles), -doubling * jnp.sin(angles)], axis=0).astype(jnp.bfloat16)

def reference(grid_state, conv_weight, spectral_gain, spectral_weight, norm_gain, expand_weight, reduce_weight):
    lat_total = grid_state.shape[0]
    values_wide = grid_state.astype(jnp.float32)
    padded = jnp.pad(values_wide, ((1, 1), (0, 0), (0, 0)))
    padded = jnp.concatenate([padded[:, -1:], padded, padded[:, :1]], axis=1)
    filtered = jnp.zeros_like(values_wide)
    for row_shift in range(3):
        for col_shift in range(3):
            filtered = filtered + conv_weight[row_shift, col_shift] * padded[row_shift:row_shift + lat_total, col_shift:col_shift + NLON]
    first_section = (values_wide + jax.nn.gelu(filtered)).astype(jnp.bfloat16)
    longitudes = jnp.arange(NLON, dtype=jnp.int32)
    forward_table = fourier_table(longitudes, NLON, M)
    spectrum = jnp.einsum('tpc,prm->tmrc', first_section.astype(jnp.float32), forward_table.astype(jnp.float32), precision=lax.Precision.HIGHEST).astype(jnp.bfloat16)
    legendre = legendre_table(jnp.arange(M, dtype=jnp.int32), lat_total, M)
    analysis_table = (legendre * quadrature(lat_total)[None, None, :]).astype(jnp.bfloat16)
    coefficients = jnp.einsum('lmt,tmrc->lmrc', analysis_table.astype(jnp.float32), spectrum.astype(jnp.float32), precision=lax.Precision.HIGHEST)
    gain_real = spectral_gain[0][:, None, :]
    gain_imag = spectral_gain[1][:, None, :]
    coef_real = coefficients[:, :, 0, :]
    coef_imag = coefficients[:, :, 1, :]
    gained = jnp.stack([gain_real * coef_real - gain_imag * coef_imag, gain_real * coef_imag + gain_imag * coef_real], axis=2).astype(jnp.bfloat16)
    real_in = gained[:, :, 0, :].astype(jnp.float32)
    imag_in = gained[:, :, 1, :].astype(jnp.float32)
    mix_real = spectral_weight[0].astype(jnp.float32)
    mix_imag = spectral_weight[1].astype(jnp.float32)
    real_out = jnp.einsum('lmc,cd->lmd', real_in, mix_real, precision=lax.Precision.HIGHEST) - jnp.einsum('lmc,cd->lmd', imag_in, mix_imag, precision=lax.Precision.HIGHEST)
    imag_out = jnp.einsum('lmc,cd->lmd', real_in, mix_imag, precision=lax.Precision.HIGHEST) + jnp.einsum('lmc,cd->lmd', imag_in, mix_real, precision=lax.Precision.HIGHEST)
    mixed = jnp.stack([real_out, imag_out], axis=2).astype(jnp.bfloat16)
    synthesis_legendre = legendre.astype(jnp.bfloat16)
    cycle_modes = jnp.einsum('lmt,lmrc->tmrc', synthesis_legendre.astype(jnp.float32), mixed.astype(jnp.float32), precision=lax.Precision.HIGHEST).astype(jnp.bfloat16)
    inverse_table = synthesis_table(longitudes, NLON, M)
    spectral_out = jnp.einsum('tmrc,rmp->tpc', cycle_modes.astype(jnp.float32), inverse_table.astype(jnp.float32), precision=lax.Precision.HIGHEST)
    second_section = (first_section.astype(jnp.float32) + spectral_out).astype(jnp.bfloat16)
    second_wide = second_section.astype(jnp.float32)
    scale_values = lax.rsqrt(lax.optimization_barrier(jnp.mean(second_wide * second_wide, axis=-1, keepdims=True)) + norm_eps)
    normed = (second_wide * norm_gain * scale_values).astype(jnp.bfloat16)
    flat_rows = normed.reshape(-1, C)
    hidden = jax.nn.gelu(jnp.dot(flat_rows, expand_weight, preferred_element_type=jnp.float32)).astype(jnp.bfloat16)
    update = jnp.dot(hidden, reduce_weight, preferred_element_type=jnp.float32)
    block_output = (second_wide.reshape(-1, C) + update).astype(jnp.bfloat16)
    return block_output.reshape(grid_state.shape)
```

```python
import functools
import math

import jax
import jax.numpy as jnp
import numpy as np
from jax import lax
from jax.experimental import pallas as pl
from jax.experimental.pallas import tpu as pltpu
from jax.sharding import PartitionSpec as P

M = 256


norm_eps = 1e-06
underflow_cut = -60.0


def padded_2(value, sides, width, wrap):
    for axis, dim in sides:
        count, length = (lax.axis_size(axis), value.shape[dim])
        up = [(i, (i + 1) % count) for i in range(count if wrap else count - 1)]
        down = [(j, i) for i, j in up]
        last = lax.slice_in_dim(value, length - width, length, axis=dim)
        initial = lax.slice_in_dim(value, 0, width, axis=dim)
        before = lax.ppermute(last, axis, up)
        after = lax.ppermute(initial, axis, down)
        value = jnp.concatenate([before, value, after], axis=dim)
    return value


def joined_along(parts, dim):
    parts = jnp.moveaxis(parts, 0, dim)
    dims = parts.shape
    return parts.reshape(*dims[:dim], dims[dim] * dims[dim + 1], *dims[dim + 2 :])


def from_everyone(value, axis):
    copies = jnp.broadcast_to(value, (lax.axis_size(axis), *value.shape))
    return lax.all_to_all(copies, axis, split_axis=0, concat_axis=0, tiled=True)


def gathered_copies(value, axis, dim):
    return joined_along(from_everyone(value, axis), dim)


def latitude_rows(lat_total):
    theta = (np.arange(lat_total) + 0.5) * (math.pi / lat_total)
    rank = np.arange(1, lat_total + 1)
    rows = np.stack(
        [
            np.cos(theta),
            np.log(np.sin(theta)),
            2.0 * math.pi * math.pi / lat_total * np.sin(theta),
            0.5 * np.log((2.0 * rank + 1.0) / (2.0 * rank)),
        ]
    )
    return np.concatenate([rows, np.zeros_like(rows)]).astype(np.float32)


def legendre_fill(order, rows_ref, raise_ref, lower_ref, table_ref):
    degrees, width = table_ref.shape
    order_float = order.astype(jnp.float32)
    cosine = rows_ref[0:1, :]
    log_sine = rows_ref[1:2, :]
    rank = lax.broadcasted_iota(jnp.int32, (1, width), 1) + 1
    log_norm = jnp.sum(jnp.where(rank <= order, rows_ref[3:4, :], 0.0), axis=1, keepdims=True)
    log_start = -0.5 * math.log(4.0 * math.pi) + log_norm + order_float * log_sine
    start = jnp.where(log_start > underflow_cut, jnp.exp(jnp.maximum(log_start, underflow_cut)), 0.0)
    degree = lax.broadcasted_iota(jnp.int32, (degrees, width), 0).astype(jnp.float32)
    raise_coef = jnp.sqrt(
        jnp.maximum(4.0 * degree * degree - 1.0, 0.0)
        / jnp.maximum(degree * degree - order_float * order_float, 1.0)
    )
    below = degree - 1.0
    lower_coef = jnp.sqrt(
        jnp.maximum(below * below - order_float * order_float, 0.0)
        / jnp.maximum(4.0 * below * below - 1.0, 1.0)
    )
    raise_ref[...] = raise_coef * cosine
    lower_ref[...] = raise_coef * lower_coef

    def advance(degree_now, carried):
        previous, earlier = carried
        row = pl.ds(degree_now, 1)
        recurred = raise_ref[row, :] * previous - lower_ref[row, :] * earlier
        current = jnp.where(degree_now == order, start, recurred)
        table_ref[row, :] = current
        return current, previous

    blank = 0.0 * raise_ref[0:1, :]
    lax.fori_loop(0, degrees, advance, (blank, blank), unroll=8)


def legendre_kernel(order_count, rows_ref, analysis_ref, synthesis_ref, raise_ref, lower_ref, table_ref):
    order = lax.axis_index("lat") * order_count + pl.program_id(0)
    legendre_fill(order, rows_ref, raise_ref, lower_ref, table_ref)
    table = table_ref[...]
    synthesis_ref[...] = table.astype(jnp.bfloat16)
    analysis_ref[...] = (table * rows_ref[2:3, :]).astype(jnp.bfloat16)


def legendre_tables(order_count, lat_total, degree_count):
    square = (degree_count, lat_total)
    block = pl.BlockSpec((None, *square), lambda i: (i, 0, 0))
    return pl.pallas_call(
        functools.partial(legendre_kernel, order_count),
        grid=(order_count,),
        in_specs=[pl.BlockSpec((8, lat_total), lambda i: (0, 0))],
        out_specs=[block, block],
        out_shape=[jax.ShapeDtypeStruct((order_count, *square), jnp.bfloat16)] * 2,
        scratch_shapes=[pltpu.VMEM(square, jnp.float32)] * 3,
        name="legendre",
    )(jnp.asarray(latitude_rows(lat_total)))


def fourier_tables(lon_total, mode_count):
    phase = np.outer(np.arange(lon_total), np.arange(mode_count)) % lon_total
    angles = phase * (2.0 * math.pi / lon_total)
    forward = np.stack([np.cos(angles), -np.sin(angles)], axis=1) / lon_total
    doubling = np.where(np.arange(mode_count) == 0, 1.0, 2.0)
    inverse = np.stack([np.cos(angles).T, -np.sin(angles).T]) * doubling[None, :, None]
    return (
        jnp.asarray(forward.astype(np.float32).astype(jnp.bfloat16)),
        jnp.asarray(inverse.astype(np.float32).astype(jnp.bfloat16)),
    )


def shards(
    grid_state, conv_weight, spectral_gain, spectral_weight, norm_gain, expand_weight, reduce_weight
):
    lat_rows, sector_width, channel_total = grid_state.shape
    lat_count = lax.axis_size("lat")
    lon_count = lax.axis_size("lon")
    lat_total = lat_rows * lat_count
    lon_total = sector_width * lon_count
    mode_count = M
    order_share = mode_count // lat_count
    channel_share = channel_total // lon_count
    wrapped = padded_2(grid_state, (("lon", 1),), 1, True)
    padded = padded_2(wrapped, (("lat", 0),), 1, False)
    padded_wide = padded.astype(jnp.float32)
    filtered = jnp.zeros((lat_rows, sector_width, channel_total), jnp.float32)
    for row_shift in range(3):
        for col_shift in range(3):
            filtered = (
                filtered
                + conv_weight[row_shift, col_shift]
                * padded_wide[
                    row_shift : row_shift + lat_rows, col_shift : col_shift + sector_width
                ]
            )
    first_section = (grid_state.astype(jnp.float32) + jax.nn.gelu(filtered)).astype(jnp.bfloat16)
    gathered = lax.all_to_all(first_section, "lon", split_axis=2, concat_axis=1, tiled=True)
    forward_table, inverse_table = fourier_tables(lon_total, mode_count)
    spectrum = jnp.einsum(
        "tpc,prm->tmrc", gathered, forward_table, preferred_element_type=jnp.float32
    ).astype(jnp.bfloat16)
    cycle_spectrum = lax.all_to_all(spectrum, "lat", split_axis=1, concat_axis=0, tiled=True)
    analysis_table, synthesis_legendre = legendre_tables(order_share, lat_total, mode_count)
    coefficients = jnp.einsum(
        "mlt,tmrc->lmrc", analysis_table, cycle_spectrum, preferred_element_type=jnp.float32
    )
    gain_real = spectral_gain[0][:, None, :]
    gain_imag = spectral_gain[1][:, None, :]
    coef_real = coefficients[:, :, 0, :]
    coef_imag = coefficients[:, :, 1, :]
    gained = jnp.stack(
        [
            gain_real * coef_real - gain_imag * coef_imag,
            gain_real * coef_imag + gain_imag * coef_real,
        ],
        axis=2,
    ).astype(jnp.bfloat16)
    blank = jnp.zeros((mode_count * order_share, channel_share), jnp.float32)
    portion = gathered_copies(gained, "lon", 3)
    width_part = portion.shape[3]
    weight_rows = lax.slice_in_dim(spectral_weight, 0, width_part, axis=1)
    real_part = portion[:, :, 0, :].reshape(-1, width_part)
    imag_part = portion[:, :, 1, :].reshape(-1, width_part)
    real_sum = (
        blank
        + jnp.dot(real_part, weight_rows[0], preferred_element_type=jnp.float32)
        - jnp.dot(imag_part, weight_rows[1], preferred_element_type=jnp.float32)
    )
    imag_sum = (
        blank
        + jnp.dot(real_part, weight_rows[1], preferred_element_type=jnp.float32)
        + jnp.dot(imag_part, weight_rows[0], preferred_element_type=jnp.float32)
    )
    mixed = jnp.stack(
        [
            real_sum.reshape(mode_count, order_share, channel_share),
            imag_sum.reshape(mode_count, order_share, channel_share),
        ],
        axis=2,
    ).astype(jnp.bfloat16)
    cycle_modes = jnp.einsum(
        "mlt,lmrc->tmrc", synthesis_legendre, mixed, preferred_element_type=jnp.float32
    ).astype(jnp.bfloat16)
    band_modes = lax.all_to_all(cycle_modes, "lat", split_axis=0, concat_axis=1, tiled=True)
    all_lons = jnp.einsum(
        "tmrc,rmp->tpc", band_modes, inverse_table, preferred_element_type=jnp.float32
    )
    spectral_out = lax.all_to_all(
        all_lons.astype(jnp.bfloat16), "lon", split_axis=1, concat_axis=2, tiled=True
    ).astype(all_lons.dtype)
    second_section = (first_section.astype(jnp.float32) + spectral_out).astype(jnp.bfloat16)
    second_wide = second_section.astype(jnp.float32)
    scale_values = lax.rsqrt(jnp.mean(second_wide * second_wide, axis=-1, keepdims=True) + norm_eps)
    normed = (second_wide * norm_gain * scale_values).astype(jnp.bfloat16)
    flat_rows = normed.reshape(-1, channel_total)
    hidden = jax.nn.gelu(
        jnp.dot(flat_rows, expand_weight, preferred_element_type=jnp.float32)
    ).astype(jnp.bfloat16)
    update = jnp.dot(hidden, reduce_weight, preferred_element_type=jnp.float32)
    block_output = (second_wide.reshape(-1, channel_total) + update).astype(jnp.bfloat16)
    return block_output.reshape(lat_rows, sector_width, channel_total)


def solution(mesh):
    return jax.shard_map(
        shards,
        mesh=mesh,
        in_specs=(
            P("lat", "lon", None),
            P(),
            P(None, None, "lon"),
            P(None, None, "lon"),
            P(),
            P(),
            P(),
        ),
        out_specs=P("lat", "lon", None),
        check_vma=False,
    )
```

```python
import functools
import math

import jax
import jax.numpy as jnp
import numpy as np
from jax import lax
from jax.experimental import pallas as pl
from jax.experimental.pallas import tpu as pltpu
from jax.sharding import PartitionSpec as P

M = 256
norm_eps = 1e-06
underflow_cut = -60.0
edge_rows = 16
bf16 = jnp.bfloat16
f32 = jnp.float32
MESH = pl.DeviceIdType.MESH


def cycle_of_row(rings, depth):
    row = np.arange(rings * depth * 4)
    plane, z = row // depth, row % depth
    return (plane // 4) * (4 * depth) + 4 * z + plane % 4


def latitude_rows(lat_total, rings, depth):
    theta = (cycle_of_row(rings, depth) + 0.5) * (math.pi / lat_total)
    rank = np.arange(1, lat_total + 1)
    rows = np.stack(
        [
            np.cos(theta),
            np.log(np.sin(theta)),
            2.0 * math.pi * math.pi / lat_total * np.sin(theta),
            0.5 * np.log((2.0 * rank + 1.0) / (2.0 * rank)),
        ]
    )
    return np.concatenate([rows, np.zeros_like(rows)]).astype(np.float32)


def fourier_tables(sector, padded, mode_count, rings, depth):
    lon_total = 4 * sector
    z, j, r = np.meshgrid(np.arange(depth), np.arange(2 * rings), np.arange(2), indexing="ij")
    z, j, r = z.ravel(), j.ravel(), r.ravel()
    column = np.arange(4 * padded)
    lon = (column // padded) * sector + column % padded
    inside = (column % padded) < sector
    forward, inverse = [], []
    for core in range(2):
        order = (2 * j + core) * depth + z
        angle = (order[:, None] * lon[None, :] % lon_total) * (2.0 * math.pi / lon_total)
        wave = np.where(r[:, None] == 0, np.cos(angle), -np.sin(angle)) * inside[None, :]
        forward.append(wave / lon_total)
        inverse.append((wave * np.where(order == 0, 1.0, 2.0)[:, None]).T)
    forward = np.stack(forward).astype(np.float32).astype(bf16)
    inverse = np.concatenate(inverse, axis=1).reshape(4, padded, mode_count * 2)
    return jnp.asarray(forward), jnp.asarray(inverse.astype(np.float32).astype(bf16))


def legendre_fill(order, rows_ref, raise_ref, lower_ref, table_ref):
    degrees, width = table_ref.shape
    order_float = order.astype(f32)
    cosine = rows_ref[0:1, :]
    log_sine = rows_ref[1:2, :]
    rank = lax.broadcasted_iota(jnp.int32, (1, width), 1) + 1
    log_norm = jnp.sum(jnp.where(rank <= order, rows_ref[3:4, :], 0.0), axis=1, keepdims=True)
    log_start = -0.5 * math.log(4.0 * math.pi) + log_norm + order_float * log_sine
    start = jnp.where(log_start > underflow_cut, jnp.exp(jnp.maximum(log_start, underflow_cut)), 0.0)
    degree = lax.broadcasted_iota(jnp.int32, (degrees, width), 0).astype(f32)
    raise_coef = jnp.sqrt(
        jnp.maximum(4.0 * degree * degree - 1.0, 0.0)
        / jnp.maximum(degree * degree - order_float * order_float, 1.0)
    )
    below = degree - 1.0
    lower_coef = jnp.sqrt(
        jnp.maximum(below * below - order_float * order_float, 0.0)
        / jnp.maximum(4.0 * below * below - 1.0, 1.0)
    )
    raise_ref[...] = raise_coef * cosine
    lower_ref[...] = raise_coef * lower_coef

    def advance(degree_now, carried):
        previous, earlier = carried
        row = pl.ds(degree_now, 1)
        recurred = raise_ref[row, :] * previous - lower_ref[row, :] * earlier
        current = jnp.where(degree_now == order, start, recurred)
        table_ref[row, :] = current
        return current, previous

    blank = 0.0 * raise_ref[0:1, :]
    lax.fori_loop(0, degrees, advance, (blank, blank), unroll=8)


def block_kernel(
    rings,
    depth,
    spans,
    grid_hbm,
    conv_ref,
    gain_hbm,
    mix_hbm,
    norm_ref,
    expand_hbm,
    reduce_hbm,
    forward_hbm,
    inverse_hbm,
    rows_ref,
    out_ref,
    grid_v,
    halo_v,
    edge_out,
    edge_in,
    wide_v,
    first_v,
    circle_v,
    modes_v,
    column_v,
    turned_v,
    meridian_v,
    coef_own,
    coef_out,
    coef_in,
    gain_part,
    gain_all,
    gain_v,
    mix_v,
    gained_v,
    mixed_out,
    mixed_v,
    cycle_v,
    back_v,
    column_back,
    modes_all,
    spectral_own,
    spectral_out,
    spectral_in,
    normed_v,
    total_v,
    expand_v,
    reduce_v,
    forward_v,
    inverse_v,
    swap_v,
    raise_v,
    lower_v,
    table_v,
    analysis_v,
    synthesis_v,
    sems,
    local_sems,
):
    sector, channels = grid_v.shape[1:]
    padded = first_v.shape[1]
    lat_count = rings * depth * 2
    swap_rows = 4 * rings
    share = mix_hbm.shape[1]
    half = coef_own.shape[0]
    lat = lax.axis_index("lat")
    lon = lax.axis_index("lon")
    x_high = lat % 2
    z = (lat // 2) % depth
    y = lat // (2 * depth)
    x_low = lon // 2
    core = lon % 2
    plane = 4 * y + 2 * x_high + x_low
    slot = (2 * y + x_high) * 2 + core
    order = plane * depth + z
    twin = lon + 1 - 2 * core
    across = (lon + 2) % 4
    opposite = 3 - lon
    lat_up = (lat + 1) % lat_count
    lat_down = (lat + lat_count - 1) % lat_count
    lat_pair = lat + 1 - 2 * x_high
    lon_up = (lon + 1) % 4
    lon_down = (lon + 3) % 4
    diagonal = core == x_low

    names = {}

    def sem(name):
        index = names.setdefault(name, len(names))
        assert index < sems.shape[0], "semaphores"
        return sems.at[index]

    def send(source, target, name, lat_to, lon_to):
        copy = pltpu.make_async_remote_copy(
            src_ref=source,
            dst_ref=target,
            send_sem=sem(name + ".s"),
            recv_sem=sem(name + ".r"),
            device_id={"lat": lat_to, "lon": lon_to},
            device_id_type=MESH,
        )
        copy.start()

    def wait(ref, semaphore):
        pltpu.make_async_copy(ref, ref, semaphore).wait()

    def arrived(ref, name):
        wait(ref, sem(name + ".r"))

    def left(ref, name):
        wait(ref, sem(name + ".s"))

    def z_offset(i):
        return depth // 2 + (1 - 2 * (i % 2)) * ((i + 1) // 2)

    def ring_peer(i):
        return (z + z_offset(i)) % depth

    def lat_of(y_to, z_to, high_to):
        return (y_to * depth + z_to) * 2 + high_to

    def order_peer(i):
        return lat_of(i // 4, z, (i // 2) % 2), 2 * core + i % 2

    def cycle_peer(i):
        return lat_of(i // 4, z, (i % 4) // 2), 2 * (i % 2) + x_low

    barrier = pltpu.get_barrier_semaphore()

    def greet(lat_to, lon_to):
        pl.semaphore_signal(
            barrier, inc=1, device_id={"lat": lat_to, "lon": lon_to}, device_id_type=MESH
        )

    for lat_to in (lat_up, lat_down):
        for lon_to in (lon, lon_up, lon_down):
            greet(lat_to, lon_to)
    greet(lat, lon_up)
    greet(lat, lon_down)
    greet(lat, across)
    greet(lat_pair, across)
    greet(lat_pair, opposite)

    @pl.loop(0, depth - 1)
    def _(i):
        greet(lat_of(y, ring_peer(i), x_high), lon)

    @pl.loop(0, swap_rows)
    def _(i):
        for peer in (order_peer, cycle_peer):
            lat_to, lon_to = peer(i)

            @pl.when(jnp.logical_or(lat_to != lat, lon_to != lon))
            def _():
                greet(lat_to, lon_to)

    loads = {}

    def load(name, source, target):
        copy = pltpu.make_async_copy(source, target, local_sems.at[len(loads)])
        copy.start()
        loads[name] = copy

    load("grid", grid_hbm, grid_v)
    mix_own = mix_v.at[:, pl.ds(pl.multiple_of(lon * share, 16), share), :]
    load("mix", mix_hbm, mix_own)
    load("gain0", gain_hbm.at[:, :, pl.ds(0, half)], gain_part.at[0])
    load("gain1", gain_hbm.at[:, :, pl.ds(half, half)], gain_part.at[1])
    load("forward", forward_hbm.at[core], forward_v)
    load("inverse0", inverse_hbm.at[lon], inverse_v.at[0])
    load("inverse1", inverse_hbm.at[across], inverse_v.at[1])
    load("expand", expand_hbm, expand_v)
    load("reduce", reduce_hbm, reduce_v)

    loads["grid"].wait()
    for t in range(2):
        edge_out[0, t] = grid_v[t, 0:edge_rows, :]
        edge_out[1, t] = grid_v[t, sector - edge_rows : sector, :]
    pl.semaphore_wait(barrier, 11 + depth - 1 + 2 * swap_rows - 2 * diagonal.astype(jnp.int32))

    for side, lon_to in ((0, lon_down), (1, lon_up)):
        send(edge_out.at[side, 1], edge_in.at[side, 0], "edge", lat_up, lon_to)
        send(edge_out.at[side, 0], edge_in.at[side, 3], "edge", lat_down, lon_to)
        send(edge_out.at[side], edge_in.at[side, pl.ds(1, 2)], "edge", lat, lon_to)
    for k, (base, width) in enumerate(spans):
        lanes = pl.ds(base, width)
        send(grid_v.at[1, :, lanes], halo_v.at[0, :, lanes], f"halo{k}", lat_up, lon)
        send(grid_v.at[0, :, lanes], halo_v.at[1, :, lanes], f"halo{k}", lat_down, lon)

    loads["mix"].wait()
    loads["gain0"].wait()
    loads["gain1"].wait()
    send(mix_own, mix_own, "mixx", lat_pair, across)
    send(mix_own, mix_own, "mixc", lat, twin)
    gain_all[lon] = gain_part[core]
    send(gain_part.at[core], gain_all.at[lon], "gain", lat_pair, across)
    send(gain_part.at[1 - core], gain_all.at[lon], "gain", lat_pair, opposite)
    send(gain_part.at[1 - core], gain_all.at[lon], "gain", lat, twin)

    side = swap_rows * depth
    row = lax.broadcasted_iota(jnp.int32, (side, side), 0)
    column = lax.broadcasted_iota(jnp.int32, (side, side), 1)
    first_v[:, padded - 16 : padded, :] = jnp.zeros((2, 16, channels), bf16)
    swap_v[0] = (column == (row % depth) * swap_rows + row // depth).astype(f32).astype(bf16)
    swap_v[1] = (column == (row % swap_rows) * depth + row // swap_rows).astype(f32).astype(bf16)
    legendre_fill(order, rows_ref, raise_v, lower_v, table_v)
    table = table_v[...]
    analysis_v[...] = (table * rows_ref[2:3, :]).astype(bf16).reshape(analysis_v.shape)
    synthesis_v[...] = table.T.astype(bf16)

    above = (lat > 0).astype(f32)
    below = (lat < lat_count - 1).astype(f32)
    scales = (above, None, None, below)

    def stage_conv(k):
        base, width = spans[k]
        lanes = pl.ds(base, width)
        if k == 0:
            arrived(edge_in, "edge")
        arrived(halo_v.at[:, :, lanes], f"halo{k}")
        for line in range(4):
            source = (halo_v.at[0], grid_v.at[0], grid_v.at[1], halo_v.at[1])[line]
            body = source[:, lanes].astype(f32)
            before = edge_in[1, line, :, lanes].astype(f32)[edge_rows - 1 :]
            after = edge_in[0, line, :, lanes].astype(f32)[:1]
            if scales[line] is not None:
                body, before, after = (scales[line] * v for v in (body, before, after))
            wide_v[line, 8 : 8 + sector, lanes] = body
            wide_v[line, 7:8, lanes] = before
            wide_v[line, 8 + sector : 9 + sector, lanes] = after
        for t in range(2):
            filtered = None
            for i in range(3):
                for j in range(3):
                    term = conv_ref[i, j : j + 1, lanes] * wide_v[t + i, 7 + j : 7 + j + sector, lanes]
                    filtered = term if filtered is None else filtered + term
            centre = wide_v[t + 1, 8 : 8 + sector, lanes]
            first_v[t, 0:sector, lanes] = (centre + jax.nn.gelu(filtered)).astype(bf16)
        send(first_v.at[1 - x_low, :, lanes], circle_v.at[lon, :, lanes], f"lonx{k}", lat, across)
        send(first_v.at[x_low, :, lanes], circle_v.at[lon, :, lanes], f"lonc{k}", lat, twin)
        circle_v[lon, :, lanes] = first_v[x_low, :, lanes]

    def stage_relay(k):
        base, width = spans[k]
        lanes = pl.ds(base, width)
        arrived(circle_v.at[across, :, lanes], f"lonx{k}")
        send(circle_v.at[across, :, lanes], circle_v.at[across, :, lanes], f"lonr{k}", lat, twin)

    def stage_fourier(k):
        base, width = spans[k]
        lanes = pl.ds(base, width)
        if k == 0:
            loads["forward"].wait()
        arrived(circle_v.at[twin, :, lanes], f"lonc{k}")
        arrived(circle_v.at[opposite, :, lanes], f"lonr{k}")
        circle = circle_v[:, :, lanes].reshape(4 * padded, width)
        modes = jnp.dot(forward_v[...], circle, preferred_element_type=f32).astype(bf16)
        modes_v[:, :, lanes] = modes.reshape(depth, swap_rows, width)

        @pl.loop(0, depth - 1)
        def _(i):
            z_to = ring_peer(i)
            send(
                modes_v.at[z_to, :, lanes],
                column_v.at[z, :, lanes],
                f"ring{k}",
                lat_of(y, z_to, x_high),
                lon,
            )

        column_v[z, :, lanes] = modes_v[z, :, lanes]

    def stage_turn(k):
        base, width = spans[k]
        lanes = pl.ds(base, width)
        arrived(column_v.at[pl.ds(0, depth - 1), :, lanes], f"ring{k}")
        column = column_v[:, :, lanes].reshape(side, width)
        turned = jnp.dot(swap_v[0], column, preferred_element_type=f32).astype(bf16)
        turned_v[:, :, lanes] = turned.reshape(swap_rows, depth, width)

        @pl.loop(0, swap_rows)
        def _(i):
            to = (slot + i) % swap_rows
            lat_to, lon_to = order_peer(to)

            @pl.when(jnp.logical_or(lat_to != lat, lon_to != lon))
            def _():
                send(
                    turned_v.at[to, :, lanes],
                    meridian_v.at[plane, :, lanes],
                    f"plane{k}",
                    lat_to,
                    lon_to,
                )

        @pl.when(diagonal)
        def _():
            meridian_v[plane, :, lanes] = turned_v[slot, :, lanes]

    def count_wait(ref, lanes, semaphore):
        @pl.when(diagonal)
        def _():
            wait(ref.at[pl.ds(0, swap_rows - 1), :, lanes], semaphore)

        @pl.when(jnp.logical_not(diagonal))
        def _():
            wait(ref.at[:, :, lanes], semaphore)

    def stage_analysis(k):
        base, width = spans[k]
        lanes = pl.ds(base, width)
        count_wait(meridian_v, lanes, sem(f"plane{k}.r"))
        meridian = meridian_v[:, :, lanes].reshape(side, width)
        coef_out[:, lanes] = jnp.dot(analysis_v[1 - core], meridian, preferred_element_type=f32)
        send(coef_out.at[:, lanes], coef_in.at[:, lanes], f"coef{k}", lat, twin)
        coef_own[:, lanes] = jnp.dot(analysis_v[core], meridian, preferred_element_type=f32)

    def stage_gain(k):
        base, width = spans[k]
        lanes = pl.ds(base, width)
        if k == 0:
            arrived(gain_all.at[pl.ds(0, 3)], "gain")
            for r in range(2):
                whole = gain_all[:, r].reshape(channels, half)
                gain_v[r] = whole.T
            arrived(mix_v.at[:, pl.ds(0, share), :], "mixx")
            opposite_mix = mix_v.at[:, pl.ds(pl.multiple_of(across * share, 16), share), :]
            send(opposite_mix, opposite_mix, "mixr", lat, twin)
        arrived(coef_in.at[:, lanes], f"coef{k}")
        own = coef_own[:, lanes]
        other = coef_in[:, lanes]
        real = jnp.where(core == 0, own, other)
        imag = jnp.where(core == 0, other, own)
        gain_real = gain_v[0, :, lanes]
        gain_imag = gain_v[1, :, lanes]
        gained_v[0:half, lanes] = (gain_real * real - gain_imag * imag).astype(bf16)
        gained_v[half : 2 * half, lanes] = (gain_real * imag + gain_imag * real).astype(bf16)

    def stage_mix(k):
        base, width = spans[k]
        lanes = pl.ds(base, width)
        if k == 0:
            arrived(mix_v.at[:, pl.ds(0, share), :], "mixc")
            arrived(mix_v.at[:, pl.ds(0, share), :], "mixr")
        gained = gained_v[...]
        contract = (((1,), (1,)), ((), ()))
        by_real = lax.dot_general(gained, mix_v[0, lanes, :], contract, preferred_element_type=f32)
        by_imag = lax.dot_general(gained, mix_v[1, lanes, :], contract, preferred_element_type=f32)
        real = by_real[:half] - by_imag[half:]
        imag = by_imag[:half] + by_real[half:]
        mixed_out[:, lanes] = jnp.where(core == 0, imag, real).astype(bf16)
        send(mixed_out.at[:, lanes], mixed_v.at[core, :, lanes], f"mixed{k}", lat, twin)
        mixed_v[core, :, lanes] = jnp.where(core == 0, real, imag).astype(bf16)

    def stage_synthesis(k):
        base, width = spans[k]
        lanes = pl.ds(base, width)
        arrived(mixed_v.at[1 - core, :, lanes], f"mixed{k}")
        mixed = mixed_v[:, :, lanes].reshape(2 * half, width)
        cycle = jnp.dot(synthesis_v[...], mixed, preferred_element_type=f32).astype(bf16)
        cycle_v[:, :, lanes] = cycle.reshape(swap_rows, depth, width)

        @pl.loop(0, swap_rows)
        def _(i):
            to = (plane + i) % swap_rows
            lat_to, lon_to = cycle_peer(to)

            @pl.when(jnp.logical_or(lat_to != lat, lon_to != lon))
            def _():
                send(
                    cycle_v.at[to, :, lanes],
                    back_v.at[slot, :, lanes],
                    f"plback{k}",
                    lat_to,
                    lon_to,
                )

        @pl.when(diagonal)
        def _():
            back_v[slot, :, lanes] = cycle_v[plane, :, lanes]

    def stage_turn_back(k):
        base, width = spans[k]
        lanes = pl.ds(base, width)
        count_wait(back_v, lanes, sem(f"plback{k}.r"))
        back = back_v[:, :, lanes].reshape(side, width)
        turned = jnp.dot(swap_v[1], back, preferred_element_type=f32).astype(bf16)
        column_back[:, :, lanes] = turned.reshape(depth, swap_rows, width)

        @pl.loop(0, depth - 1)
        def _(i):
            z_to = ring_peer(i)
            send(
                column_back.at[z_to, :, lanes],
                modes_all.at[core, z, :, lanes],
                f"rgback{k}",
                lat_of(y, z_to, x_high),
                lon,
            )

        modes_all[core, z, :, lanes] = column_back[z, :, lanes]

    def stage_share(k):
        base, width = spans[k]
        lanes = pl.ds(base, width)
        arrived(modes_all.at[core, pl.ds(0, depth - 1), :, lanes], f"rgback{k}")
        send(modes_all.at[core, :, :, lanes], modes_all.at[core, :, :, lanes], f"modes{k}", lat, twin)

    def stage_inverse(k):
        base, width = spans[k]
        lanes = pl.ds(base, width)
        if k == 0:
            loads["inverse0"].wait()
            loads["inverse1"].wait()
        arrived(modes_all.at[1 - core, :, :, lanes], f"modes{k}")
        modes = modes_all[:, :, :, lanes].reshape(2 * side, width)
        spectral_out[:, lanes] = jnp.dot(
            inverse_v[1], modes, preferred_element_type=f32
        ).astype(bf16)
        send(spectral_out.at[:, lanes], spectral_in.at[:, lanes], f"spec{k}", lat, across)
        spectral_own[:, lanes] = jnp.dot(inverse_v[0], modes, preferred_element_type=f32)

    def finish(which, spectral):
        second = (first_v[which].astype(f32) + spectral).astype(bf16).astype(f32)
        scale = lax.rsqrt(jnp.mean(second * second, axis=-1, keepdims=True) + norm_eps)
        normed_v[...] = (second * norm_ref[...] * scale).astype(bf16)
        total_v[...] = second
        hidden_width = expand_v.shape[1]
        step = min(256, hidden_width)
        for base in range(0, hidden_width, step):
            columns = slice(base, base + step)
            hidden = jax.nn.gelu(
                jnp.dot(normed_v[...], expand_v[:, columns], preferred_element_type=f32)
            ).astype(bf16)
            total_v[...] += jnp.dot(hidden, reduce_v[columns, :], preferred_element_type=f32)
        out_ref[which] = total_v[0:sector, :].astype(bf16)

    def pipeline(stages):
        count = len(spans)
        for beat in range(count + len(stages) - 1):
            for depth_now, stage in enumerate(stages):
                k = beat - depth_now
                if 0 <= k < count:
                    stage(k)

    pipeline([stage_conv, stage_relay, stage_fourier, stage_turn, stage_analysis, stage_gain])
    pipeline([stage_mix, stage_synthesis, stage_turn_back, stage_share, stage_inverse])

    loads["expand"].wait()
    loads["reduce"].wait()
    finish(x_low, spectral_own[...])
    for k, (base, width) in enumerate(spans):
        arrived(spectral_in.at[:, pl.ds(base, width)], f"spec{k}")
    finish(1 - x_low, spectral_in[...].astype(f32))

    left(edge_in, "edge")
    left(mix_v.at[:, pl.ds(0, share), :], "mixx")
    left(mix_v.at[:, pl.ds(0, share), :], "mixc")
    left(mix_v.at[:, pl.ds(0, share), :], "mixr")
    left(gain_all.at[pl.ds(0, 3)], "gain")
    for k, (base, width) in enumerate(spans):
        lanes = pl.ds(base, width)
        left(halo_v.at[:, :, lanes], f"halo{k}")
        for name in ("lonx", "lonc", "lonr"):
            left(circle_v.at[0, :, lanes], f"{name}{k}")
        left(column_v.at[pl.ds(0, depth - 1), :, lanes], f"ring{k}")
        count_wait(meridian_v, lanes, sem(f"plane{k}.s"))
        left(coef_in.at[:, lanes], f"coef{k}")
        left(mixed_out.at[:, lanes], f"mixed{k}")
        count_wait(back_v, lanes, sem(f"plback{k}.s"))
        left(column_v.at[pl.ds(0, depth - 1), :, lanes], f"rgback{k}")
        left(modes_all.at[0, :, :, lanes], f"modes{k}")
        left(spectral_out.at[:, lanes], f"spec{k}")


def spans_of(channels, pieces):
    tiles = channels // 128
    cuts = [tiles * i // pieces for i in range(pieces + 1)]
    return [(128 * a, 128 * (b - a)) for a, b in zip(cuts, cuts[1:])]


chunk_count = 1


def shards(
    rings,
    depth,
    grid_state,
    conv_weight,
    spectral_gain,
    spectral_weight,
    norm_gain,
    expand_weight,
    reduce_weight,
):
    two, sector, channels = grid_state.shape
    padded = -(-sector // 16) * 16
    degrees = spectral_gain.shape[1]
    lat_total = 4 * rings * depth
    side = lat_total
    swap_rows = 4 * rings
    half = degrees // 2
    share = channels // 4
    hidden_width = expand_weight.shape[1]
    spans = spans_of(channels, chunk_count)
    forward, inverse = fourier_tables(sector, padded, degrees, rings, depth)
    rows = jnp.asarray(latitude_rows(lat_total, rings, depth))
    anywhere = pl.BlockSpec(memory_space=pl.ANY)
    vmem = pl.BlockSpec(memory_space=pltpu.VMEM)
    scratch = [
        ((2, sector, channels), bf16),
        ((2, sector, channels), bf16),
        ((2, 2, edge_rows, channels), bf16),
        ((2, 4, edge_rows, channels), bf16),
        ((4, -(-(sector + 16) // 8) * 8, channels), f32),
        ((2, padded, channels), bf16),
        ((4, padded, channels), bf16),
        ((depth, swap_rows, channels), bf16),
        ((depth, swap_rows, channels), bf16),
        ((swap_rows, depth, channels), bf16),
        ((swap_rows, depth, channels), bf16),
        ((half, channels), f32),
        ((half, channels), f32),
        ((half, channels), f32),
        ((2, 2, share, half), f32),
        ((4, 2, share, half), f32),
        ((2, half, channels), f32),
        ((2, channels, channels), bf16),
        ((2 * half, channels), bf16),
        ((half, channels), bf16),
        ((2, half, channels), bf16),
        ((swap_rows, depth, channels), bf16),
        ((swap_rows, depth, channels), bf16),
        ((depth, swap_rows, channels), bf16),
        ((2, depth, swap_rows, channels), bf16),
        ((padded, channels), f32),
        ((padded, channels), bf16),
        ((padded, channels), bf16),
        ((padded, channels), bf16),
        ((padded, channels), f32),
        ((channels, hidden_width), bf16),
        ((hidden_width, channels), bf16),
        ((side, 4 * padded), bf16),
        ((2, padded, 2 * side), bf16),
        ((2, side, side), bf16),
        ((degrees, lat_total), f32),
        ((degrees, lat_total), f32),
        ((degrees, lat_total), f32),
        ((2, half, lat_total), bf16),
        ((lat_total, degrees), bf16),
    ]
    return pl.pallas_call(
        functools.partial(block_kernel, rings, depth, spans),
        out_shape=jax.ShapeDtypeStruct(grid_state.shape, bf16),
        in_specs=[anywhere, vmem, anywhere, anywhere, vmem] + [anywhere] * 4 + [vmem],
        out_specs=vmem,
        scratch_shapes=[pltpu.VMEM(*s) for s in scratch]
        + [
            pltpu.SemaphoreType.DMA((10 + 24 * len(spans),)),
            pltpu.SemaphoreType.DMA((9,)),
        ],
        compiler_params=pltpu.CompilerParams(
            collective_id=0, has_side_effects=True, vmem_limit_bytes=60 * 1024 * 1024
        ),
        name="block_pair",
    )(
        grid_state,
        conv_weight,
        jnp.swapaxes(spectral_gain, 1, 2),
        jnp.swapaxes(spectral_weight, 1, 2),
        norm_gain.reshape(1, channels),
        expand_weight,
        reduce_weight,
        forward,
        inverse,
        rows,
    )


def solution(mesh):
    lat_count = mesh.shape["lat"]
    rings = max(1, lat_count // 32)
    depth = lat_count // (2 * rings)
    return jax.shard_map(
        functools.partial(shards, rings, depth),
        mesh=mesh,
        in_specs=(
            P("lat", "lon", None),
            P(),
            P(None, None, "lon"),
            P(None, None, "lon"),
            P(),
            P(),
            P(),
        ),
        out_specs=P("lat", "lon", None),
        check_vma=False,
    )
```

```python
import functools
import math

import jax
import jax.numpy as jnp
import numpy as np
from jax import lax
from jax.experimental import pallas as pl
from jax.experimental.pallas import tpu as pltpu
from jax.sharding import PartitionSpec as P

M = 256
norm_eps = 1e-06
underflow_cut = -60.0
edge_rows = 16
bf16 = jnp.bfloat16
f32 = jnp.float32
MESH = pl.DeviceIdType.MESH


def cycle_of_row(rings, depth):
    row = np.arange(rings * depth * 4)
    plane, z = row // depth, row % depth
    return (plane // 4) * (4 * depth) + 4 * z + plane % 4


def latitude_rows(lat_total, rings, depth):
    theta = (cycle_of_row(rings, depth) + 0.5) * (math.pi / lat_total)
    rank = np.arange(1, lat_total + 1)
    rows = np.stack(
        [
            np.cos(theta),
            np.log(np.sin(theta)),
            2.0 * math.pi * math.pi / lat_total * np.sin(theta),
            0.5 * np.log((2.0 * rank + 1.0) / (2.0 * rank)),
        ]
    )
    return np.concatenate([rows, np.zeros_like(rows)]).astype(np.float32)


def fourier_tables(sector, padded, mode_count, rings, depth):
    lon_total = 4 * sector
    z, j, r = np.meshgrid(np.arange(depth), np.arange(2 * rings), np.arange(2), indexing="ij")
    z, j, r = z.ravel(), j.ravel(), r.ravel()
    column = np.arange(4 * padded)
    lon = (column // padded) * sector + column % padded
    inside = (column % padded) < sector
    forward, inverse = [], []
    for core in range(2):
        order = (2 * j + core) * depth + z
        angle = (order[:, None] * lon[None, :] % lon_total) * (2.0 * math.pi / lon_total)
        wave = np.where(r[:, None] == 0, np.cos(angle), -np.sin(angle)) * inside[None, :]
        forward.append(wave / lon_total)
        inverse.append((wave * np.where(order == 0, 1.0, 2.0)[:, None]).T)
    forward = np.stack(forward).astype(np.float32).astype(bf16)
    inverse = np.concatenate(inverse, axis=1).reshape(4, padded, mode_count * 2)
    return jnp.asarray(forward), jnp.asarray(inverse.astype(np.float32).astype(bf16))


def legendre_fill(order, rows_ref, raise_ref, lower_ref, table_ref):
    degrees, width = table_ref.shape
    order_float = order.astype(f32)
    cosine = rows_ref[0:1, :]
    log_sine = rows_ref[1:2, :]
    rank = lax.broadcasted_iota(jnp.int32, (1, width), 1) + 1
    log_norm = jnp.sum(jnp.where(rank <= order, rows_ref[3:4, :], 0.0), axis=1, keepdims=True)
    log_start = -0.5 * math.log(4.0 * math.pi) + log_norm + order_float * log_sine
    start = jnp.where(log_start > underflow_cut, jnp.exp(jnp.maximum(log_start, underflow_cut)), 0.0)
    degree = lax.broadcasted_iota(jnp.int32, (degrees, width), 0).astype(f32)
    raise_coef = jnp.sqrt(
        jnp.maximum(4.0 * degree * degree - 1.0, 0.0)
        / jnp.maximum(degree * degree - order_float * order_float, 1.0)
    )
    below = degree - 1.0
    lower_coef = jnp.sqrt(
        jnp.maximum(below * below - order_float * order_float, 0.0)
        / jnp.maximum(4.0 * below * below - 1.0, 1.0)
    )
    raise_ref[...] = raise_coef * cosine
    lower_ref[...] = raise_coef * lower_coef

    def advance(degree_now, carried):
        previous, earlier = carried
        row = pl.ds(degree_now, 1)
        recurred = raise_ref[row, :] * previous - lower_ref[row, :] * earlier
        current = jnp.where(degree_now == order, start, recurred)
        table_ref[row, :] = current
        return current, previous

    blank = 0.0 * raise_ref[0:1, :]
    lax.fori_loop(0, degrees, advance, (blank, blank), unroll=8)


def block_kernel(
    rings,
    depth,
    spans,
    spans_back,
    grid_hbm,
    conv_hbm,
    gain_hbm,
    mix_hbm,
    norm_hbm,
    expand_hbm,
    reduce_hbm,
    forward_hbm,
    inverse_hbm,
    rows_hbm,
    out_hbm,
    conv_ref,
    norm_ref,
    rows_ref,
    out_ref,
    grid_v,
    halo_v,
    edge_out,
    edge_in,
    wide_v,
    first_v,
    circle_v,
    modes_v,
    column_v,
    turned_v,
    meridian_v,
    coef_own,
    coef_out,
    coef_in,
    gain_part,
    gain_all,
    gain_v,
    mix_v,
    gained_v,
    mixed_out,
    mixed_v,
    cycle_v,
    back_v,
    column_back,
    modes_all,
    spectral_own,
    spectral_out,
    spectral_in,
    normed_v,
    total_v,
    expand_v,
    reduce_v,
    forward_v,
    inverse_v,
    swap_v,
    raise_v,
    lower_v,
    table_v,
    analysis_v,
    synthesis_v,
    sems,
    local_sems,
):
    sector, channels = grid_v.shape[1:]
    padded = first_v.shape[1]
    lat_count = rings * depth * 2
    swap_rows = 4 * rings
    share = mix_hbm.shape[1]
    half = coef_own.shape[0]
    lat = lax.axis_index("lat")
    lon = lax.axis_index("lon")
    x_high = lat % 2
    z = (lat // 2) % depth
    y = lat // (2 * depth)
    x_low = lon // 2
    core = lon % 2
    plane = 4 * y + 2 * x_high + x_low
    slot = (2 * y + x_high) * 2 + core
    order = plane * depth + z
    twin = lon + 1 - 2 * core
    across = (lon + 2) % 4
    opposite = 3 - lon
    lat_up = (lat + 1) % lat_count
    lat_down = (lat + lat_count - 1) % lat_count
    lat_pair = lat + 1 - 2 * x_high
    lon_up = (lon + 1) % 4
    lon_down = (lon + 3) % 4
    diagonal = core == x_low

    names = {}

    def sem(name):
        index = names.setdefault(name, len(names))
        assert index < sems.shape[0], "semaphores"
        return sems.at[index]

    def send(source, target, name, lat_to, lon_to):
        copy = pltpu.make_async_remote_copy(
            src_ref=source,
            dst_ref=target,
            send_sem=sem(name + ".s"),
            recv_sem=sem(name + ".r"),
            device_id={"lat": lat_to, "lon": lon_to},
            device_id_type=MESH,
        )
        copy.start()

    def wait(ref, semaphore):
        pltpu.make_async_copy(ref, ref, semaphore).wait()

    def arrived(ref, name):
        wait(ref, sem(name + ".r"))

    def left(ref, name):
        wait(ref, sem(name + ".s"))

    def z_offset(i):
        return depth // 2 + (1 - 2 * (i % 2)) * ((i + 1) // 2)

    def ring_peer(i):
        return (z + z_offset(i)) % depth

    def lat_of(y_to, z_to, high_to):
        return (y_to * depth + z_to) * 2 + high_to

    def order_peer(i):
        return lat_of(i // 4, z, (i // 2) % 2), 2 * core + i % 2

    def cycle_peer(i):
        return lat_of(i // 4, z, (i % 4) // 2), 2 * (i % 2) + x_low

    barrier = pltpu.get_barrier_semaphore()

    def greet(lat_to, lon_to):
        pl.semaphore_signal(
            barrier, inc=1, device_id={"lat": lat_to, "lon": lon_to}, device_id_type=MESH
        )

    for lat_to in (lat_up, lat_down):
        for lon_to in (lon, lon_up, lon_down):
            greet(lat_to, lon_to)
    greet(lat, lon_up)
    greet(lat, lon_down)
    greet(lat, across)
    greet(lat_pair, across)
    greet(lat_pair, opposite)

    @pl.loop(0, depth - 1)
    def _(i):
        greet(lat_of(y, ring_peer(i), x_high), lon)

    @pl.loop(0, swap_rows)
    def _(i):
        for peer in (order_peer, cycle_peer):
            lat_to, lon_to = peer(i)

            @pl.when(jnp.logical_or(lat_to != lat, lon_to != lon))
            def _():
                greet(lat_to, lon_to)

    loads = {}

    def load(name, source, target):
        copy = pltpu.make_async_copy(source, target, local_sems.at[len(loads)])
        copy.start()
        loads[name] = copy

    load("grid", grid_hbm, grid_v)
    load("rows", rows_hbm, rows_ref)
    load("conv", conv_hbm, conv_ref)
    load("norm", norm_hbm, norm_ref)
    mix_own = mix_v.at[:, pl.ds(pl.multiple_of(lon * share, 16), share), :]
    load("mix", mix_hbm, mix_own)
    load("gain0", gain_hbm.at[:, :, pl.ds(0, half)], gain_part.at[0])
    load("gain1", gain_hbm.at[:, :, pl.ds(half, half)], gain_part.at[1])
    load("forward", forward_hbm.at[core], forward_v)
    load("inverse0", inverse_hbm.at[lon], inverse_v.at[0])
    load("inverse1", inverse_hbm.at[across], inverse_v.at[1])
    load("expand", expand_hbm, expand_v)
    load("reduce", reduce_hbm, reduce_v)

    loads["grid"].wait()
    blank = jnp.zeros((8 - channels // 128, 128), f32)
    for side, at in ((0, 0), (1, sector - 8)):
        pieces = []
        for t in range(2):
            line = grid_v[t, at : at + 8, :].astype(f32)[7 * side : 7 * side + 1]
            pieces += [line[:, base : base + 128] for base in range(0, channels, 128)] + [blank]
        edge_out[side] = jnp.concatenate(pieces, axis=0).astype(bf16)
    pl.semaphore_wait(barrier, 11 + depth - 1 + 2 * swap_rows - 2 * diagonal.astype(jnp.int32))

    for side, lon_to in ((0, lon_down), (1, lon_up)):
        for source, lat_to in ((0, lat_up), (1, lat), (2, lat_down)):
            send(edge_out.at[side], edge_in.at[side, source], "edge", lat_to, lon_to)
    def stage_halo(k):
        base, width = spans[k]
        lanes = pl.ds(base, width)
        send(grid_v.at[1, :, lanes], halo_v.at[0, :, lanes], f"halo{k}", lat_up, lon)
        send(grid_v.at[0, :, lanes], halo_v.at[1, :, lanes], f"halo{k}", lat_down, lon)

    ahead = min(halo_ahead, len(spans))
    for k in range(ahead):
        stage_halo(k)

    side = swap_rows * depth
    row = lax.broadcasted_iota(jnp.int32, (side, side), 0)
    column = lax.broadcasted_iota(jnp.int32, (side, side), 1)
    first_v[:, padded - 16 : padded, :] = jnp.zeros((2, 16, channels), bf16)
    swap_v[0] = (column == (row % depth) * swap_rows + row // depth).astype(f32).astype(bf16)
    swap_v[1] = (column == (row % swap_rows) * depth + row // swap_rows).astype(f32).astype(bf16)
    loads["rows"].wait()
    loads["conv"].wait()
    loads["norm"].wait()
    legendre_fill(order, rows_ref, raise_v, lower_v, table_v)
    table = table_v[...]
    analysis_v[...] = (table * rows_ref[2:3, :]).astype(bf16).reshape(analysis_v.shape)
    synthesis_v[...] = table.T.astype(bf16)

    above = (lat > 0).astype(f32)
    below = (lat < lat_count - 1).astype(f32)
    scales = (above, None, None, below)

    def edge_line(side, line, base, width):
        block = edge_in[side, (line + 1) // 2].astype(f32)
        row = 8 * (1 - line % 2) + base // 128
        return jnp.concatenate([block[i : i + 1] for i in range(row, row + width // 128)], axis=1)

    def stage_conv(k):
        base, width = spans[k]
        lanes = pl.ds(base, width)
        if k == 0:
            arrived(edge_in, "edge")
        arrived(halo_v.at[:, :, lanes], f"halo{k}")
        for line in range(4):
            source = (halo_v.at[0], grid_v.at[0], grid_v.at[1], halo_v.at[1])[line]
            body = source[:, lanes].astype(f32)
            after, before = (edge_line(side, line, base, width) for side in range(2))
            if scales[line] is not None:
                body, before, after = (scales[line] * v for v in (body, before, after))
            wide_v[line, 8 : 8 + sector, lanes] = body
            wide_v[line, 7:8, lanes] = before
            wide_v[line, 8 + sector : 9 + sector, lanes] = after
        for t in range(2):
            filtered = None
            for i in range(3):
                for j in range(3):
                    term = conv_ref[i, j : j + 1, lanes] * wide_v[t + i, 7 + j : 7 + j + sector, lanes]
                    filtered = term if filtered is None else filtered + term
            centre = wide_v[t + 1, 8 : 8 + sector, lanes]
            first_v[t, 0:sector, lanes] = (centre + jax.nn.gelu(filtered)).astype(bf16)
        send(first_v.at[1 - x_low, :, lanes], circle_v.at[lon, :, lanes], f"lonx{k}", lat, across)
        send(first_v.at[x_low, :, lanes], circle_v.at[lon, :, lanes], f"lonc{k}", lat, twin)
        circle_v[lon, :, lanes] = first_v[x_low, :, lanes]
        if k + ahead < len(spans):
            stage_halo(k + ahead)

    def send_weights():
        loads["mix"].wait()
        loads["gain0"].wait()
        loads["gain1"].wait()
        gain_all[lon] = gain_part[core]
        rows = pl.ds(pl.multiple_of(lon * share, 16), share)
        for i, lat_to in ((0, lat_pair), (1, lat)):
            part = mix_v.at[i, rows, :]
            send(part, part, "mixx", lat_to, across)
            send(gain_part.at[core, i], gain_all.at[lon, i], "gain", lat_to, across)
            send(gain_part.at[1 - core, i], gain_all.at[lon, i], "gain", lat_to, opposite)
        send(mix_own, mix_own, "mixc", lat, twin)
        send(gain_part.at[1 - core], gain_all.at[lon], "gain", lat, twin)

    def stage_relay(k):
        base, width = spans[k]
        lanes = pl.ds(base, width)
        arrived(circle_v.at[across, :, lanes], f"lonx{k}")
        send(circle_v.at[across, :, lanes], circle_v.at[across, :, lanes], f"lonr{k}", lat, twin)

    def stage_fourier(k):
        base, width = spans[k]
        lanes = pl.ds(base, width)
        if k == 0:
            loads["forward"].wait()
        arrived(circle_v.at[twin, :, lanes], f"lonc{k}")
        arrived(circle_v.at[opposite, :, lanes], f"lonr{k}")
        circle = circle_v[:, :, lanes].reshape(4 * padded, width)
        modes = jnp.dot(forward_v[...], circle, preferred_element_type=f32).astype(bf16)
        modes_v[:, :, lanes] = modes.reshape(depth, swap_rows, width)

        @pl.loop(0, depth - 1)
        def _(i):
            z_to = ring_peer(i)
            send(
                modes_v.at[z_to, :, lanes],
                column_v.at[z, :, lanes],
                f"ring{k}",
                lat_of(y, z_to, x_high),
                lon,
            )

        column_v[z, :, lanes] = modes_v[z, :, lanes]

    def stage_turn(k):
        base, width = spans[k]
        lanes = pl.ds(base, width)
        arrived(column_v.at[pl.ds(0, depth - 1), :, lanes], f"ring{k}")
        column = column_v[:, :, lanes].reshape(side, width)
        turned = jnp.dot(swap_v[0], column, preferred_element_type=f32).astype(bf16)
        turned_v[:, :, lanes] = turned.reshape(swap_rows, depth, width)

        @pl.loop(0, swap_rows)
        def _(i):
            to = (slot + i) % swap_rows
            lat_to, lon_to = order_peer(to)

            @pl.when(jnp.logical_or(lat_to != lat, lon_to != lon))
            def _():
                send(
                    turned_v.at[to, :, lanes],
                    meridian_v.at[plane, :, lanes],
                    f"plane{k}",
                    lat_to,
                    lon_to,
                )

        @pl.when(diagonal)
        def _():
            meridian_v[plane, :, lanes] = turned_v[slot, :, lanes]

    def count_wait(ref, lanes, semaphore):
        @pl.when(diagonal)
        def _():
            wait(ref.at[pl.ds(0, swap_rows - 1), :, lanes], semaphore)

        @pl.when(jnp.logical_not(diagonal))
        def _():
            wait(ref.at[:, :, lanes], semaphore)

    def stage_analysis(k):
        base, width = spans[k]
        lanes = pl.ds(base, width)
        if k == 0:
            arrived(mix_v.at[:, pl.ds(0, share), :], "mixx")
            opposite_mix = mix_v.at[:, pl.ds(pl.multiple_of(across * share, 16), share), :]
            send(opposite_mix, opposite_mix, "mixr", lat, twin)
        count_wait(meridian_v, lanes, sem(f"plane{k}.r"))
        meridian = meridian_v[:, :, lanes].reshape(side, width)
        coef_out[:, lanes] = jnp.dot(analysis_v[1 - core], meridian, preferred_element_type=f32)
        send(coef_out.at[:, lanes], coef_in.at[:, lanes], f"coef{k}", lat, twin)
        coef_own[:, lanes] = jnp.dot(analysis_v[core], meridian, preferred_element_type=f32)

    def stage_gain(k):
        base, width = spans[k]
        lanes = pl.ds(base, width)
        if k == 0:
            arrived(gain_all.at[pl.ds(0, 3)], "gain")
            for r in range(2):
                whole = gain_all[:, r].reshape(channels, half)
                gain_v[r] = whole.T
        arrived(coef_in.at[:, lanes], f"coef{k}")
        own = coef_own[:, lanes]
        other = coef_in[:, lanes]
        real = jnp.where(core == 0, own, other)
        imag = jnp.where(core == 0, other, own)
        gain_real = gain_v[0, :, lanes]
        gain_imag = gain_v[1, :, lanes]
        gained_v[0:half, lanes] = (gain_real * real - gain_imag * imag).astype(bf16)
        gained_v[half : 2 * half, lanes] = (gain_real * imag + gain_imag * real).astype(bf16)

    def stage_mix(k):
        base, width = spans_back[k]
        lanes = pl.ds(base, width)
        if k == 0:
            arrived(mix_v.at[:, pl.ds(0, share), :], "mixc")
            arrived(mix_v.at[:, pl.ds(0, share), :], "mixr")
        gained = gained_v[...]
        contract = (((1,), (1,)), ((), ()))
        by_real = lax.dot_general(gained, mix_v[0, lanes, :], contract, preferred_element_type=f32)
        by_imag = lax.dot_general(gained, mix_v[1, lanes, :], contract, preferred_element_type=f32)
        real = by_real[:half] - by_imag[half:]
        imag = by_imag[:half] + by_real[half:]
        mixed_out[:, lanes] = jnp.where(core == 0, imag, real).astype(bf16)
        send(mixed_out.at[:, lanes], mixed_v.at[core, :, lanes], f"mixed{k}", lat, twin)
        mixed_v[core, :, lanes] = jnp.where(core == 0, real, imag).astype(bf16)

    def stage_synthesis(k):
        base, width = spans_back[k]
        lanes = pl.ds(base, width)
        arrived(mixed_v.at[1 - core, :, lanes], f"mixed{k}")
        mixed = mixed_v[:, :, lanes].reshape(2 * half, width)
        cycle = jnp.dot(synthesis_v[...], mixed, preferred_element_type=f32).astype(bf16)
        cycle_v[:, :, lanes] = cycle.reshape(swap_rows, depth, width)

        @pl.loop(0, swap_rows)
        def _(i):
            to = (plane + i) % swap_rows
            lat_to, lon_to = cycle_peer(to)

            @pl.when(jnp.logical_or(lat_to != lat, lon_to != lon))
            def _():
                send(
                    cycle_v.at[to, :, lanes],
                    back_v.at[slot, :, lanes],
                    f"plback{k}",
                    lat_to,
                    lon_to,
                )

        @pl.when(diagonal)
        def _():
            back_v[slot, :, lanes] = cycle_v[plane, :, lanes]

    def stage_turn_back(k):
        base, width = spans_back[k]
        lanes = pl.ds(base, width)
        count_wait(back_v, lanes, sem(f"plback{k}.r"))
        back = back_v[:, :, lanes].reshape(side, width)
        turned = jnp.dot(swap_v[1], back, preferred_element_type=f32).astype(bf16)
        column_back[:, :, lanes] = turned.reshape(depth, swap_rows, width)

        @pl.loop(0, depth - 1)
        def _(i):
            z_to = ring_peer(i)
            send(
                column_back.at[z_to, :, lanes],
                modes_all.at[core, z, :, lanes],
                f"rgback{k}",
                lat_of(y, z_to, x_high),
                lon,
            )

        modes_all[core, z, :, lanes] = column_back[z, :, lanes]

    def stage_share(k):
        base, width = spans_back[k]
        lanes = pl.ds(base, width)
        arrived(modes_all.at[core, pl.ds(0, depth - 1), :, lanes], f"rgback{k}")
        send(modes_all.at[core, :, :, lanes], modes_all.at[core, :, :, lanes], f"modes{k}", lat, twin)

    def stage_inverse(k):
        base, width = spans_back[k]
        lanes = pl.ds(base, width)
        if k == 0:
            loads["inverse0"].wait()
            loads["inverse1"].wait()
        arrived(modes_all.at[1 - core, :, :, lanes], f"modes{k}")
        modes = modes_all[:, :, :, lanes].reshape(2 * side, width)
        spectral_out[:, lanes] = jnp.dot(
            inverse_v[1], modes, preferred_element_type=f32
        ).astype(bf16)
        send(spectral_out.at[:, lanes], spectral_in.at[:, lanes], f"spec{k}", lat, across)
        spectral_own[:, lanes] = jnp.dot(inverse_v[0], modes, preferred_element_type=f32)

    def finish(which, spectral):
        second = (first_v[which].astype(f32) + spectral).astype(bf16).astype(f32)
        scale = lax.rsqrt(jnp.mean(second * second, axis=-1, keepdims=True) + norm_eps)
        normed_v[...] = (second * norm_ref[...].reshape(1, channels) * scale).astype(bf16)
        total_v[...] = second
        hidden_width = expand_v.shape[1]
        step = min(256, hidden_width)
        for base in range(0, hidden_width, step):
            columns = slice(base, base + step)
            hidden = jax.nn.gelu(
                jnp.dot(normed_v[...], expand_v[:, columns], preferred_element_type=f32)
            ).astype(bf16)
            total_v[...] += jnp.dot(hidden, reduce_v[columns, :], preferred_element_type=f32)
        out_ref[which] = total_v[0:sector, :].astype(bf16)
        load(f"out{len(loads)}", out_ref.at[which], out_hbm.at[which])

    def run(count, stages, lags):
        for beat in range(count + max(lags)):
            for stage, lag in reversed(list(zip(stages, lags))):
                if 0 <= beat - lag < count:
                    stage(beat - lag)

    count = len(spans)
    run(count, [stage_conv, stage_relay, stage_fourier], front_lags)
    send_weights()
    run(count, [stage_turn, stage_analysis, stage_gain], [0, count, 2 * count])
    count = len(spans_back)
    late = [stage_mix, stage_synthesis, stage_turn_back, stage_share, stage_inverse]
    run(count, late, [0, count, 2 * count, 3 * count, 3 * count + 1])

    loads["expand"].wait()
    loads["reduce"].wait()
    finish(x_low, spectral_own[...])
    for k, (base, width) in enumerate(spans_back):
        arrived(spectral_in.at[:, pl.ds(base, width)], f"spec{k}")
    finish(1 - x_low, spectral_in[...].astype(f32))

    for name, copy in loads.items():
        if name.startswith("out"):
            copy.wait()
    left(edge_in, "edge")
    left(mix_v.at[:, pl.ds(0, share), :], "mixx")
    left(mix_v.at[:, pl.ds(0, share), :], "mixc")
    left(mix_v.at[:, pl.ds(0, share), :], "mixr")
    left(gain_all.at[pl.ds(0, 3)], "gain")
    for k, (base, width) in enumerate(spans):
        lanes = pl.ds(base, width)
        left(halo_v.at[:, :, lanes], f"halo{k}")
        for name in ("lonx", "lonc", "lonr"):
            left(circle_v.at[0, :, lanes], f"{name}{k}")
        left(column_v.at[pl.ds(0, depth - 1), :, lanes], f"ring{k}")
        count_wait(meridian_v, lanes, sem(f"plane{k}.s"))
        left(coef_in.at[:, lanes], f"coef{k}")
    for k, (base, width) in enumerate(spans_back):
        lanes = pl.ds(base, width)
        left(mixed_out.at[:, lanes], f"mixed{k}")
        count_wait(back_v, lanes, sem(f"plback{k}.s"))
        left(column_v.at[pl.ds(0, depth - 1), :, lanes], f"rgback{k}")
        left(modes_all.at[0, :, :, lanes], f"modes{k}")
        left(spectral_out.at[:, lanes], f"spec{k}")


def spans_of(tiles):
    edges = np.concatenate([[0], np.cumsum(tiles)]) * 128
    return [(int(a), int(b - a)) for a, b in zip(edges, edges[1:])]


front_tiles = (1, 2, 2)
back_tiles = (2, 2, 1)
halo_ahead = 2
front_lags = (0, 1, 2)


def shards(
    rings,
    depth,
    grid_state,
    conv_weight,
    spectral_gain,
    spectral_weight,
    norm_gain,
    expand_weight,
    reduce_weight,
):
    two, sector, channels = grid_state.shape
    padded = -(-sector // 16) * 16
    degrees = spectral_gain.shape[1]
    lat_total = 4 * rings * depth
    side = lat_total
    swap_rows = 4 * rings
    half = degrees // 2
    share = channels // 4
    hidden_width = expand_weight.shape[1]
    spans, spans_back = spans_of(front_tiles), spans_of(back_tiles)
    forward, inverse = fourier_tables(sector, padded, degrees, rings, depth)
    rows = jnp.asarray(latitude_rows(lat_total, rings, depth))
    anywhere = pl.BlockSpec(memory_space=pl.ANY)
    scratch = [
        (conv_weight.shape, f32),
        (norm_gain.shape, f32),
        (rows.shape, f32),
        (grid_state.shape, bf16),
        ((2, sector, channels), bf16),
        ((2, sector, channels), bf16),
        ((2, edge_rows, 128), bf16),
        ((2, 3, edge_rows, 128), bf16),
        ((4, -(-(sector + 16) // 8) * 8, channels), f32),
        ((2, padded, channels), bf16),
        ((4, padded, channels), bf16),
        ((depth, swap_rows, channels), bf16),
        ((depth, swap_rows, channels), bf16),
        ((swap_rows, depth, channels), bf16),
        ((swap_rows, depth, channels), bf16),
        ((half, channels), f32),
        ((half, channels), f32),
        ((half, channels), f32),
        ((2, 2, share, half), f32),
        ((4, 2, share, half), f32),
        ((2, half, channels), f32),
        ((2, channels, channels), bf16),
        ((2 * half, channels), bf16),
        ((half, channels), bf16),
        ((2, half, channels), bf16),
        ((swap_rows, depth, channels), bf16),
        ((swap_rows, depth, channels), bf16),
        ((depth, swap_rows, channels), bf16),
        ((2, depth, swap_rows, channels), bf16),
        ((padded, channels), f32),
        ((padded, channels), bf16),
        ((padded, channels), bf16),
        ((padded, channels), bf16),
        ((padded, channels), f32),
        ((channels, hidden_width), bf16),
        ((hidden_width, channels), bf16),
        ((side, 4 * padded), bf16),
        ((2, padded, 2 * side), bf16),
        ((2, side, side), bf16),
        ((degrees, lat_total), f32),
        ((degrees, lat_total), f32),
        ((degrees, lat_total), f32),
        ((2, half, lat_total), bf16),
        ((lat_total, degrees), bf16),
    ]
    return pl.pallas_call(
        functools.partial(block_kernel, rings, depth, spans, spans_back),
        out_shape=jax.ShapeDtypeStruct(grid_state.shape, bf16),
        in_specs=[anywhere] * 10,
        out_specs=anywhere,
        scratch_shapes=[pltpu.VMEM(*s) for s in scratch]
        + [
            pltpu.SemaphoreType.DMA((10 + 14 * len(spans) + 10 * len(spans_back),)),
            pltpu.SemaphoreType.DMA((14,)),
        ],
        compiler_params=pltpu.CompilerParams(
            collective_id=0, has_side_effects=True, vmem_limit_bytes=60 * 1024 * 1024
        ),
        name="block_pair",
    )(
        grid_state,
        conv_weight,
        jnp.swapaxes(spectral_gain, 1, 2),
        jnp.swapaxes(spectral_weight, 1, 2),
        norm_gain,
        expand_weight,
        reduce_weight,
        forward,
        inverse,
        rows,
    )


def solution(mesh):
    lat_count = mesh.shape["lat"]
    rings = max(1, lat_count // 32)
    depth = lat_count // (2 * rings)
    return jax.shard_map(
        functools.partial(shards, rings, depth),
        mesh=mesh,
        in_specs=(
            P("lat", "lon", None),
            P(),
            P(None, None, "lon"),
            P(None, None, "lon"),
            P(),
            P(),
            P(),
        ),
        out_specs=P("lat", "lon", None),
        check_vma=False,
    )
```

```python
import functools
import math

import jax
import jax.numpy as jnp
import numpy as np
from jax import lax
from jax.experimental import pallas as pl
from jax.experimental.pallas import tpu as pltpu
from jax.sharding import PartitionSpec as P

M = 256
norm_eps = 1e-06
underflow_cut = -60.0
edge_rows = 16
bf16 = jnp.bfloat16
f32 = jnp.float32
MESH = pl.DeviceIdType.MESH


def div(a, b):
    return lax.div(a, jnp.int32(b))


def rem(a, b):
    return lax.rem(a, jnp.int32(b))


def cycle_of_row(rings, depth):
    row = np.arange(rings * depth * 4)
    plane, z = row // depth, row % depth
    return (plane // 4) * (4 * depth) + 4 * z + plane % 4


def latitude_rows(lat_total, rings, depth):
    theta = (cycle_of_row(rings, depth) + 0.5) * (math.pi / lat_total)
    rank = np.arange(1, lat_total + 1)
    rows = np.stack(
        [
            np.cos(theta),
            np.log(np.sin(theta)),
            2.0 * math.pi * math.pi / lat_total * np.sin(theta),
            0.5 * np.log((2.0 * rank + 1.0) / (2.0 * rank)),
        ]
    )
    return np.concatenate([rows, np.zeros_like(rows)]).astype(np.float32)


def fourier_tables(sector, padded, mode_count, rings, depth):
    lon_total = 4 * sector
    z, j, r = np.meshgrid(np.arange(depth), np.arange(2 * rings), np.arange(2), indexing="ij")
    z, j, r = z.ravel(), j.ravel(), r.ravel()
    column = np.arange(4 * padded)
    lon = (column // padded) * sector + column % padded
    inside = (column % padded) < sector
    forward, inverse = [], []
    for core in range(2):
        order = (2 * j + core) * depth + z
        angle = (order[:, None] * lon[None, :] % lon_total) * (2.0 * math.pi / lon_total)
        wave = np.where(r[:, None] == 0, np.cos(angle), -np.sin(angle)) * inside[None, :]
        forward.append(wave / lon_total)
        inverse.append((wave * np.where(order == 0, 1.0, 2.0)[:, None]).T)
    forward = np.stack(forward).astype(np.float32).astype(bf16)
    inverse = np.concatenate(inverse, axis=1).reshape(4, padded, mode_count * 2)
    return jnp.asarray(forward), jnp.asarray(inverse.astype(np.float32).astype(bf16))


def legendre_fill(order, rows_ref, raise_ref, lower_ref, table_ref):
    degrees, width = table_ref.shape
    order_float = order.astype(f32)
    cosine = rows_ref[0:1, :]
    log_sine = rows_ref[1:2, :]
    rank = lax.broadcasted_iota(jnp.int32, (1, width), 1) + 1
    log_norm = jnp.sum(jnp.where(rank <= order, rows_ref[3:4, :], 0.0), axis=1, keepdims=True)
    log_start = -0.5 * math.log(4.0 * math.pi) + log_norm + order_float * log_sine
    start = jnp.where(log_start > underflow_cut, jnp.exp(jnp.maximum(log_start, underflow_cut)), 0.0)
    degree = lax.broadcasted_iota(jnp.int32, (degrees, width), 0).astype(f32)
    raise_coef = jnp.sqrt(
        jnp.maximum(4.0 * degree * degree - 1.0, 0.0)
        / jnp.maximum(degree * degree - order_float * order_float, 1.0)
    )
    below = degree - 1.0
    lower_coef = jnp.sqrt(
        jnp.maximum(below * below - order_float * order_float, 0.0)
        / jnp.maximum(4.0 * below * below - 1.0, 1.0)
    )
    raise_ref[...] = raise_coef * cosine
    lower_ref[...] = raise_coef * lower_coef

    def advance(degree_now, carried):
        previous, earlier = carried
        row = pl.ds(degree_now, 1)
        recurred = raise_ref[row, :] * previous - lower_ref[row, :] * earlier
        current = jnp.where(degree_now == order, start, recurred)
        table_ref[row, :] = current
        return current, previous

    blank = 0.0 * raise_ref[0:1, :]
    lax.fori_loop(0, degrees, advance, (blank, blank), unroll=8)


def block_kernel(
    rings,
    depth,
    spans,
    spans_back,
    grid_hbm,
    conv_hbm,
    gain_hbm,
    mix_hbm,
    norm_hbm,
    expand_hbm,
    reduce_hbm,
    forward_hbm,
    inverse_hbm,
    rows_hbm,
    out_hbm,
    conv_ref,
    norm_ref,
    rows_ref,
    done_v,
    out_ref,
    raw_v,
    grid_v,
    halo_v,
    edge_out,
    edge_in,
    wide_v,
    first_v,
    circle_v,
    modes_v,
    column_v,
    turned_v,
    meridian_v,
    coef_own,
    coef_out,
    coef_in,
    gain_part,
    gain_all,
    gain_v,
    mix_v,
    gained_v,
    mixed_out,
    mixed_v,
    cycle_v,
    back_v,
    column_back,
    modes_all,
    spectral_own,
    spectral_out,
    spectral_in,
    normed_v,
    total_v,
    expand_v,
    reduce_v,
    forward_v,
    inverse_v,
    swap_v,
    raise_v,
    lower_v,
    table_v,
    analysis_v,
    synthesis_v,
    sems,
    local_sems,
    far_sems,
):
    sector, channels = grid_v.shape[1:]
    padded = first_v.shape[1]
    lat_count = rings * depth * 2
    swap_rows = 4 * rings
    share = mix_hbm.shape[1]
    half = coef_own.shape[0]
    lat = lax.axis_index("lat")
    lon = lax.axis_index("lon")
    x_high = rem(lat, 2)
    z = rem(div(lat, 2), depth)
    y = div(lat, 2 * depth)
    x_low = div(lon, 2)
    core = rem(lon, 2)
    plane = 4 * y + 2 * x_high + x_low
    slot = (2 * y + x_high) * 2 + core
    order = plane * depth + z
    twin = lon + 1 - 2 * core
    across = rem(lon + 2, 4)
    opposite = 3 - lon
    lat_up = rem(lat + 1, lat_count)
    lat_down = rem(lat + lat_count - 1, lat_count)
    lat_pair = lat + 1 - 2 * x_high
    lon_up = rem(lon + 1, 4)
    lon_down = rem(lon + 3, 4)
    diagonal = core == x_low

    names = {}

    def sem(name):
        index = names.setdefault(name, len(names))
        assert index < sems.shape[0], "semaphores"
        return sems.at[index]

    def send(source, target, name, lat_to, lon_to):
        copy = pltpu.make_async_remote_copy(
            src_ref=source,
            dst_ref=target,
            send_sem=sem(name + ".s"),
            recv_sem=sem(name + ".r"),
            device_id={"lat": lat_to, "lon": lon_to},
            device_id_type=MESH,
        )
        copy.start()

    def wait(ref, semaphore):
        pltpu.make_async_copy(ref, ref, semaphore).wait()

    def arrived(ref, name):
        wait(ref, sem(name + ".r"))

    def left(ref, name):
        wait(ref, sem(name + ".s"))

    def z_offset(i):
        return depth // 2 + (1 - 2 * rem(i, 2)) * div(i + 1, 2)

    def ring_peer(i):
        return rem(z + z_offset(i), depth)

    def lat_of(y_to, z_to, high_to):
        return (y_to * depth + z_to) * 2 + high_to

    def order_peer(i):
        return lat_of(div(i, 4), z, rem(div(i, 2), 2)), 2 * core + rem(i, 2)

    def cycle_peer(i):
        return lat_of(div(i, 4), z, rem(div(i, 2), 2)), 2 * rem(i, 2) + x_low

    loads = {}

    def load(name, source, target):
        copy = pltpu.make_async_copy(source, target, local_sems.at[len(loads)])
        copy.start()
        loads[name] = copy

    load("grid", grid_hbm, raw_v)
    load("rows", rows_hbm, rows_ref)
    load("conv", conv_hbm, conv_ref)
    load("norm", norm_hbm, norm_ref)
    mix_own = mix_v.at[:, pl.ds(pl.multiple_of(lon * share, 16), share), :]
    load("mix", mix_hbm, mix_own)
    load("gain0", gain_hbm.at[:, :, pl.ds(0, half)], gain_part.at[0])
    load("gain1", gain_hbm.at[:, :, pl.ds(half, half)], gain_part.at[1])
    load("forward", forward_hbm.at[core], forward_v)
    load("inverse0", inverse_hbm.at[lon], inverse_v.at[0])
    load("inverse1", inverse_hbm.at[across], inverse_v.at[1])
    load("expand", expand_hbm, expand_v)
    load("reduce", reduce_hbm, reduce_v)

    barrier = pltpu.get_barrier_semaphore()

    def greet(lat_to, lon_to):
        pl.semaphore_signal(
            barrier, inc=1, device_id={"lat": lat_to, "lon": lon_to}, device_id_type=MESH
        )

    for lat_to in (lat_up, lat_down):
        for lon_to in (lon, lon_up, lon_down):
            greet(lat_to, lon_to)
    greet(lat, lon_up)
    greet(lat, lon_down)
    greet(lat, across)
    greet(lat_pair, across)
    greet(lat_pair, opposite)

    for step in (1, depth - 1):
        greet(lat_of(y, rem(z + step, depth), x_high), lon)

    @pl.loop(0, swap_rows)
    def _(i):
        for peer in (order_peer, cycle_peer):
            lat_to, lon_to = peer(i)

            @pl.when(jnp.logical_or(lat_to != lat, lon_to != lon))
            def _():
                greet(lat_to, lon_to)

    loads["grid"].wait()
    for t in range(2):
        grid_v[t] = raw_v[:, t, :]
    blank = jnp.zeros((8 - channels // 128, 128), f32)
    for side, at in ((0, 0), (1, sector - 8)):
        pieces = []
        for t in range(2):
            line = grid_v[t, at : at + 8, :].astype(f32)[7 * side : 7 * side + 1]
            pieces += [line[:, base : base + 128] for base in range(0, channels, 128)] + [blank]
        edge_out[side] = jnp.concatenate(pieces, axis=0).astype(bf16)
    pl.semaphore_wait(barrier, 13 + 2 * swap_rows - 2 * diagonal.astype(jnp.int32))

    far_steps = [2**i for i in range(depth.bit_length()) if 2**i < depth // 2]

    def tell(i):
        for step in (far_steps[i], depth - far_steps[i]):
            pl.semaphore_signal(
                far_sems.at[i],
                inc=1,
                device_id={"lat": lat_of(y, rem(z + step, depth), x_high), "lon": lon},
                device_id_type=MESH,
            )

    def hear(i):
        pl.semaphore_wait(far_sems.at[i], 2)

    if far_steps:
        tell(0)
    for side, lon_to in ((0, lon_down), (1, lon_up)):
        for source, lat_to in ((0, lat_up), (1, lat), (2, lat_down)):
            send(edge_out.at[side], edge_in.at[side, source], "edge", lat_to, lon_to)
    def stage_halo(k):
        base, width = spans[k]
        lanes = pl.ds(base, width)
        send(grid_v.at[1, :, lanes], halo_v.at[0, :, lanes], f"halo{k}", lat_up, lon)
        send(grid_v.at[0, :, lanes], halo_v.at[1, :, lanes], f"halo{k}", lat_down, lon)

    ahead = min(halo_ahead, len(spans))
    for k in range(ahead):
        stage_halo(k)

    side = swap_rows * depth
    row = lax.broadcasted_iota(jnp.int32, (side, side), 0)
    column = lax.broadcasted_iota(jnp.int32, (side, side), 1)
    first_v[:, padded - 16 : padded, :] = jnp.zeros((2, 16, channels), bf16)
    swap_v[0] = (column == (row % depth) * swap_rows + row // depth).astype(f32).astype(bf16)
    swap_v[1] = (column == (row % swap_rows) * depth + row // swap_rows).astype(f32).astype(bf16)
    loads["rows"].wait()
    loads["conv"].wait()
    loads["norm"].wait()
    legendre_fill(order, rows_ref, raise_v, lower_v, table_v)
    table = table_v[...]
    analysis_v[...] = (table * rows_ref[2:3, :]).astype(bf16).reshape(analysis_v.shape)
    synthesis_v[...] = table.T.astype(bf16)

    for i in range(1, len(far_steps)):
        hear(i - 1)
        tell(i)

    above = (lat > 0).astype(f32)
    below = (lat < lat_count - 1).astype(f32)
    scales = (above, None, None, below)

    def edge_line(side, line, base, width):
        block = edge_in[side, (line + 1) // 2].astype(f32)
        row = 8 * (1 - line % 2) + base // 128
        return jnp.concatenate([block[i : i + 1] for i in range(row, row + width // 128)], axis=1)

    def stage_conv(k):
        base, width = spans[k]
        lanes = pl.ds(base, width)
        if k == 0:
            arrived(edge_in, "edge")
        arrived(halo_v.at[:, :, lanes], f"halo{k}")
        for line in range(4):
            source = (halo_v.at[0], grid_v.at[0], grid_v.at[1], halo_v.at[1])[line]
            body = source[:, lanes].astype(f32)
            after, before = (edge_line(side, line, base, width) for side in range(2))
            if scales[line] is not None:
                body, before, after = (scales[line] * v for v in (body, before, after))
            wide_v[line, 8 : 8 + sector, lanes] = body
            wide_v[line, 7:8, lanes] = before
            wide_v[line, 8 + sector : 9 + sector, lanes] = after
        for t in range(2):
            filtered = None
            for i in range(3):
                for j in range(3):
                    term = conv_ref[i, j : j + 1, lanes] * wide_v[t + i, 7 + j : 7 + j + sector, lanes]
                    filtered = term if filtered is None else filtered + term
            centre = wide_v[t + 1, 8 : 8 + sector, lanes]
            first_v[t, 0:sector, lanes] = (centre + jax.nn.gelu(filtered)).astype(bf16)
        send(first_v.at[1 - x_low, :, lanes], circle_v.at[lon, :, lanes], f"lonx{k}", lat, across)
        send(first_v.at[x_low, :, lanes], circle_v.at[lon, :, lanes], f"lonc{k}", lat, twin)
        circle_v[lon, :, lanes] = first_v[x_low, :, lanes]
        if k + ahead < len(spans):
            stage_halo(k + ahead)

    def send_weights():
        loads["mix"].wait()
        loads["gain0"].wait()
        loads["gain1"].wait()
        gain_all[lon] = gain_part[core]
        rows = pl.ds(pl.multiple_of(lon * share, 16), share)
        for i, lat_to in ((0, lat_pair), (1, lat)):
            part = mix_v.at[i, rows, :]
            send(part, part, "mixx", lat_to, across)
            send(gain_part.at[core, i], gain_all.at[lon, i], "gain", lat_to, across)
            send(gain_part.at[1 - core, i], gain_all.at[lon, i], "gain", lat_to, opposite)
        send(mix_own, mix_own, "mixc", lat, twin)
        send(gain_part.at[1 - core], gain_all.at[lon], "gain", lat, twin)

    def stage_relay(k):
        base, width = spans[k]
        lanes = pl.ds(base, width)
        arrived(circle_v.at[across, :, lanes], f"lonx{k}")
        send(circle_v.at[across, :, lanes], circle_v.at[across, :, lanes], f"lonr{k}", lat, twin)

    def stage_fourier(k):
        base, width = spans[k]
        lanes = pl.ds(base, width)
        if k == 0:
            loads["forward"].wait()
            if far_steps:
                hear(len(far_steps) - 1)
        arrived(circle_v.at[twin, :, lanes], f"lonc{k}")
        arrived(circle_v.at[opposite, :, lanes], f"lonr{k}")
        circle = circle_v[:, :, lanes].reshape(4 * padded, width)
        modes = jnp.dot(forward_v[...], circle, preferred_element_type=f32).astype(bf16)
        modes_v[:, :, lanes] = modes.reshape(depth, swap_rows, width)

        @pl.loop(0, depth - 1)
        def _(i):
            z_to = ring_peer(i)
            send(
                modes_v.at[z_to, :, lanes],
                column_v.at[z, :, lanes],
                f"ring{k}",
                lat_of(y, z_to, x_high),
                lon,
            )

        column_v[z, :, lanes] = modes_v[z, :, lanes]

    def stage_turn(k):
        base, width = spans[k]
        lanes = pl.ds(base, width)
        arrived(column_v.at[pl.ds(0, depth - 1), :, lanes], f"ring{k}")
        column = column_v[:, :, lanes].reshape(side, width)
        turned = jnp.dot(swap_v[0], column, preferred_element_type=f32).astype(bf16)
        turned_v[:, :, lanes] = turned.reshape(swap_rows, depth, width)

        @pl.loop(0, swap_rows)
        def _(i):
            to = rem(slot + i, swap_rows)
            lat_to, lon_to = order_peer(to)

            @pl.when(jnp.logical_or(lat_to != lat, lon_to != lon))
            def _():
                send(
                    turned_v.at[to, :, lanes],
                    meridian_v.at[plane, :, lanes],
                    f"plane{k}",
                    lat_to,
                    lon_to,
                )

        @pl.when(diagonal)
        def _():
            meridian_v[plane, :, lanes] = turned_v[slot, :, lanes]

    def count_wait(ref, lanes, semaphore):
        @pl.when(diagonal)
        def _():
            wait(ref.at[pl.ds(0, swap_rows - 1), :, lanes], semaphore)

        @pl.when(jnp.logical_not(diagonal))
        def _():
            wait(ref.at[:, :, lanes], semaphore)

    def stage_analysis(k):
        base, width = spans[k]
        lanes = pl.ds(base, width)
        if k == 0:
            arrived(mix_v.at[:, pl.ds(0, share), :], "mixx")
            opposite_mix = mix_v.at[:, pl.ds(pl.multiple_of(across * share, 16), share), :]
            send(opposite_mix, opposite_mix, "mixr", lat, twin)
        count_wait(meridian_v, lanes, sem(f"plane{k}.r"))
        meridian = meridian_v[:, :, lanes].reshape(side, width)
        coef_out[:, lanes] = jnp.dot(analysis_v[1 - core], meridian, preferred_element_type=f32)
        send(coef_out.at[:, lanes], coef_in.at[:, lanes], f"coef{k}", lat, twin)
        coef_own[:, lanes] = jnp.dot(analysis_v[core], meridian, preferred_element_type=f32)

    def stage_gain(k):
        base, width = spans[k]
        lanes = pl.ds(base, width)
        if k == 0:
            arrived(gain_all.at[pl.ds(0, 3)], "gain")
            for r in range(2):
                whole = gain_all[:, r].reshape(channels, half)
                gain_v[r] = whole.T
        arrived(coef_in.at[:, lanes], f"coef{k}")
        own = coef_own[:, lanes]
        other = coef_in[:, lanes]
        real = jnp.where(core == 0, own, other)
        imag = jnp.where(core == 0, other, own)
        gain_real = gain_v[0, :, lanes]
        gain_imag = gain_v[1, :, lanes]
        gained_v[0:half, lanes] = (gain_real * real - gain_imag * imag).astype(bf16)
        gained_v[half : 2 * half, lanes] = (gain_real * imag + gain_imag * real).astype(bf16)

    def stage_mix(k):
        base, width = spans_back[k]
        lanes = pl.ds(base, width)
        if k == 0:
            arrived(mix_v.at[:, pl.ds(0, share), :], "mixc")
            arrived(mix_v.at[:, pl.ds(0, share), :], "mixr")
        gained = gained_v[...]
        contract = (((1,), (1,)), ((), ()))
        by_real = lax.dot_general(gained, mix_v[0, lanes, :], contract, preferred_element_type=f32)
        by_imag = lax.dot_general(gained, mix_v[1, lanes, :], contract, preferred_element_type=f32)
        real = by_real[:half] - by_imag[half:]
        imag = by_imag[:half] + by_real[half:]
        mixed_out[:, lanes] = jnp.where(core == 0, imag, real).astype(bf16)
        send(mixed_out.at[:, lanes], mixed_v.at[core, :, lanes], f"mixed{k}", lat, twin)
        mixed_v[core, :, lanes] = jnp.where(core == 0, real, imag).astype(bf16)

    def stage_synthesis(k):
        base, width = spans_back[k]
        lanes = pl.ds(base, width)
        arrived(mixed_v.at[1 - core, :, lanes], f"mixed{k}")
        mixed = mixed_v[:, :, lanes].reshape(2 * half, width)
        cycle = jnp.dot(synthesis_v[...], mixed, preferred_element_type=f32).astype(bf16)
        cycle_v[:, :, lanes] = cycle.reshape(swap_rows, depth, width)

        @pl.loop(0, swap_rows)
        def _(i):
            to = rem(plane + i, swap_rows)
            lat_to, lon_to = cycle_peer(to)

            @pl.when(jnp.logical_or(lat_to != lat, lon_to != lon))
            def _():
                send(
                    cycle_v.at[to, :, lanes],
                    back_v.at[slot, :, lanes],
                    f"plback{k}",
                    lat_to,
                    lon_to,
                )

        @pl.when(diagonal)
        def _():
            back_v[slot, :, lanes] = cycle_v[plane, :, lanes]

    def stage_turn_back(k):
        base, width = spans_back[k]
        lanes = pl.ds(base, width)
        count_wait(back_v, lanes, sem(f"plback{k}.r"))
        back = back_v[:, :, lanes].reshape(side, width)
        turned = jnp.dot(swap_v[1], back, preferred_element_type=f32).astype(bf16)
        column_back[:, :, lanes] = turned.reshape(depth, swap_rows, width)

        @pl.loop(0, depth - 1)
        def _(i):
            z_to = ring_peer(i)
            send(
                column_back.at[z_to, :, lanes],
                modes_all.at[core, z, :, lanes],
                f"rgback{k}",
                lat_of(y, z_to, x_high),
                lon,
            )

        modes_all[core, z, :, lanes] = column_back[z, :, lanes]

    def stage_share(k):
        base, width = spans_back[k]
        lanes = pl.ds(base, width)
        arrived(modes_all.at[core, pl.ds(0, depth - 1), :, lanes], f"rgback{k}")
        send(modes_all.at[core, :, :, lanes], modes_all.at[core, :, :, lanes], f"modes{k}", lat, twin)

    def stage_inverse(k):
        base, width = spans_back[k]
        lanes = pl.ds(base, width)
        if k == 0:
            loads["inverse0"].wait()
            loads["inverse1"].wait()
        arrived(modes_all.at[1 - core, :, :, lanes], f"modes{k}")
        modes = modes_all[:, :, :, lanes].reshape(2 * side, width)
        spectral_out[:, lanes] = jnp.dot(
            inverse_v[1], modes, preferred_element_type=f32
        ).astype(bf16)
        send(spectral_out.at[:, lanes], spectral_in.at[:, lanes], f"spec{k}", lat, across)
        spectral_own[:, lanes] = jnp.dot(inverse_v[0], modes, preferred_element_type=f32)

    def finish(which, spectral):
        second = (first_v[which].astype(f32) + spectral).astype(bf16).astype(f32)
        scale = lax.rsqrt(jnp.mean(second * second, axis=-1, keepdims=True) + norm_eps)
        normed_v[...] = (second * norm_ref[...].reshape(1, channels) * scale).astype(bf16)
        total_v[...] = second
        hidden_width = expand_v.shape[1]
        step = min(256, hidden_width)
        for base in range(0, hidden_width, step):
            columns = slice(base, base + step)
            hidden = jax.nn.gelu(
                jnp.dot(normed_v[...], expand_v[:, columns], preferred_element_type=f32)
            ).astype(bf16)
            total_v[...] += jnp.dot(hidden, reduce_v[columns, :], preferred_element_type=f32)
        done_v[which] = total_v[...].astype(bf16)

    def run(count, stages, lags):
        for beat in range(count + max(lags)):
            for stage, lag in reversed(list(zip(stages, lags))):
                if 0 <= beat - lag < count:
                    stage(beat - lag)

    count = len(spans)
    run(count, [stage_conv, stage_relay, stage_fourier], front_lags)
    send_weights()
    run(count, [stage_turn, stage_analysis, stage_gain], [0, count, 2 * count])
    count = len(spans_back)
    late = [stage_mix, stage_synthesis, stage_turn_back, stage_share, stage_inverse]
    run(count, late, [0, count, 2 * count, 3 * count, 3 * count + 1])

    loads["expand"].wait()
    loads["reduce"].wait()
    finish(x_low, spectral_own[...])
    for k, (base, width) in enumerate(spans_back):
        arrived(spectral_in.at[:, pl.ds(base, width)], f"spec{k}")
    finish(1 - x_low, spectral_in[...].astype(f32))

    for t in range(2):
        out_ref[:, t, :] = done_v[t, 0:sector, :]
    load("out", out_ref, out_hbm)
    loads["out"].wait()
    left(edge_in, "edge")
    left(mix_v.at[:, pl.ds(0, share), :], "mixx")
    left(mix_v.at[:, pl.ds(0, share), :], "mixc")
    left(mix_v.at[:, pl.ds(0, share), :], "mixr")
    left(gain_all.at[pl.ds(0, 3)], "gain")
    for k, (base, width) in enumerate(spans):
        lanes = pl.ds(base, width)
        left(halo_v.at[:, :, lanes], f"halo{k}")
        for name in ("lonx", "lonc", "lonr"):
            left(circle_v.at[0, :, lanes], f"{name}{k}")
        left(column_v.at[pl.ds(0, depth - 1), :, lanes], f"ring{k}")
        count_wait(meridian_v, lanes, sem(f"plane{k}.s"))
        left(coef_in.at[:, lanes], f"coef{k}")
    for k, (base, width) in enumerate(spans_back):
        lanes = pl.ds(base, width)
        left(mixed_out.at[:, lanes], f"mixed{k}")
        count_wait(back_v, lanes, sem(f"plback{k}.s"))
        left(column_v.at[pl.ds(0, depth - 1), :, lanes], f"rgback{k}")
        left(modes_all.at[0, :, :, lanes], f"modes{k}")
        left(spectral_out.at[:, lanes], f"spec{k}")


def spans_of(tiles):
    edges = np.concatenate([[0], np.cumsum(tiles)]) * 128
    return [(int(a), int(b - a)) for a, b in zip(edges, edges[1:])]


front_tiles = (1, 2, 2)
back_tiles = (2, 2, 1)
halo_ahead = 2
front_lags = (0, 1, 2)


def shards(
    rings,
    depth,
    grid_state,
    conv_weight,
    spectral_gain,
    spectral_weight,
    norm_gain,
    expand_weight,
    reduce_weight,
):
    two, sector, channels = grid_state.shape
    padded = -(-sector // 16) * 16
    degrees = spectral_gain.shape[1]
    lat_total = 4 * rings * depth
    side = lat_total
    swap_rows = 4 * rings
    half = degrees // 2
    share = channels // 4
    hidden_width = expand_weight.shape[1]
    spans, spans_back = spans_of(front_tiles), spans_of(back_tiles)
    forward, inverse = fourier_tables(sector, padded, degrees, rings, depth)
    rows = jnp.asarray(latitude_rows(lat_total, rings, depth))
    anywhere = pl.BlockSpec(memory_space=pl.ANY)
    scratch = [
        (conv_weight.shape, f32),
        (norm_gain.shape, f32),
        (rows.shape, f32),
        ((2, padded, channels), bf16),
        ((sector, 2, channels), bf16),
        ((sector, 2, channels), bf16),
        ((2, sector, channels), bf16),
        ((2, sector, channels), bf16),
        ((2, edge_rows, 128), bf16),
        ((2, 3, edge_rows, 128), bf16),
        ((4, -(-(sector + 16) // 8) * 8, channels), f32),
        ((2, padded, channels), bf16),
        ((4, padded, channels), bf16),
        ((depth, swap_rows, channels), bf16),
        ((depth, swap_rows, channels), bf16),
        ((swap_rows, depth, channels), bf16),
        ((swap_rows, depth, channels), bf16),
        ((half, channels), f32),
        ((half, channels), f32),
        ((half, channels), f32),
        ((2, 2, share, half), f32),
        ((4, 2, share, half), f32),
        ((2, half, channels), f32),
        ((2, channels, channels), bf16),
        ((2 * half, channels), bf16),
        ((half, channels), bf16),
        ((2, half, channels), bf16),
        ((swap_rows, depth, channels), bf16),
        ((swap_rows, depth, channels), bf16),
        ((depth, swap_rows, channels), bf16),
        ((2, depth, swap_rows, channels), bf16),
        ((padded, channels), f32),
        ((padded, channels), bf16),
        ((padded, channels), bf16),
        ((padded, channels), bf16),
        ((padded, channels), f32),
        ((channels, hidden_width), bf16),
        ((hidden_width, channels), bf16),
        ((side, 4 * padded), bf16),
        ((2, padded, 2 * side), bf16),
        ((2, side, side), bf16),
        ((degrees, lat_total), f32),
        ((degrees, lat_total), f32),
        ((degrees, lat_total), f32),
        ((2, half, lat_total), bf16),
        ((lat_total, degrees), bf16),
    ]
    block_output = pl.pallas_call(
        functools.partial(block_kernel, rings, depth, spans, spans_back),
        out_shape=jax.ShapeDtypeStruct((sector, 2, channels), bf16),
        in_specs=[anywhere] * 10,
        out_specs=anywhere,
        scratch_shapes=[pltpu.VMEM(*s) for s in scratch]
        + [
            pltpu.SemaphoreType.DMA((10 + 14 * len(spans) + 10 * len(spans_back),)),
            pltpu.SemaphoreType.DMA((14,)),
            pltpu.SemaphoreType.REGULAR((max(1, depth.bit_length()),)),
        ],
        compiler_params=pltpu.CompilerParams(
            collective_id=0, has_side_effects=True, vmem_limit_bytes=60 * 1024 * 1024
        ),
        name="block_pair",
    )(
        jnp.swapaxes(grid_state, 0, 1),
        conv_weight,
        jnp.swapaxes(spectral_gain, 1, 2),
        jnp.swapaxes(spectral_weight, 1, 2),
        norm_gain,
        expand_weight,
        reduce_weight,
        forward,
        inverse,
        rows,
    )
    return jnp.swapaxes(block_output, 0, 1)


def solution(mesh):
    lat_count = mesh.shape["lat"]
    rings = max(1, lat_count // 32)
    depth = lat_count // (2 * rings)
    return jax.shard_map(
        functools.partial(shards, rings, depth),
        mesh=mesh,
        in_specs=(
            P("lat", "lon", None),
            P(),
            P(None, None, "lon"),
            P(None, None, "lon"),
            P(),
            P(),
            P(),
        ),
        out_specs=P("lat", "lon", None),
        check_vma=False,
    )
```

```python
import functools
import math

import jax
import jax.numpy as jnp
import numpy as np
from jax import lax
from jax.experimental import pallas as pl
from jax.experimental.pallas import tpu as pltpu
from jax.sharding import PartitionSpec as P

M = 256
norm_eps = 1e-06
underflow_cut = -60.0
edge_rows = 16
bf16 = jnp.bfloat16
f32 = jnp.float32
MESH = pl.DeviceIdType.MESH


def div(a, b):
    return lax.div(a, jnp.int32(b))


def rem(a, b):
    return lax.rem(a, jnp.int32(b))


def cycle_of_row(rings, depth):
    row = np.arange(rings * depth * 4)
    plane, z = row // depth, row % depth
    return (plane // 4) * (4 * depth) + 4 * z + plane % 4


def latitude_rows(lat_total, rings, depth):
    theta = (cycle_of_row(rings, depth) + 0.5) * (math.pi / lat_total)
    rank = np.arange(1, lat_total + 1)
    rows = np.stack(
        [
            np.cos(theta),
            np.log(np.sin(theta)),
            2.0 * math.pi * math.pi / lat_total * np.sin(theta),
            0.5 * np.log((2.0 * rank + 1.0) / (2.0 * rank)),
        ]
    )
    return np.concatenate([rows, np.zeros_like(rows)]).astype(np.float32)


def fourier_tables(sector, padded, mode_count, rings, depth):
    lon_total = 4 * sector
    z, j, r = np.meshgrid(np.arange(depth), np.arange(2 * rings), np.arange(2), indexing="ij")
    z, j, r = z.ravel(), j.ravel(), r.ravel()
    column = np.arange(4 * padded)
    lon = (column // padded) * sector + column % padded
    inside = (column % padded) < sector
    forward, inverse = [], []
    for core in range(2):
        order = (2 * j + core) * depth + z
        angle = (order[:, None] * lon[None, :] % lon_total) * (2.0 * math.pi / lon_total)
        wave = np.where(r[:, None] == 0, np.cos(angle), -np.sin(angle)) * inside[None, :]
        forward.append(wave / lon_total)
        inverse.append((wave * np.where(order == 0, 1.0, 2.0)[:, None]).T)
    forward = np.stack(forward).astype(np.float32).astype(bf16)
    inverse = np.concatenate(inverse, axis=1).reshape(4, padded, mode_count * 2)
    return jnp.asarray(forward), jnp.asarray(inverse.astype(np.float32).astype(bf16))


def legendre_fill(order, rows_ref, raise_ref, lower_ref, table_ref):
    degrees, width = table_ref.shape
    order_float = order.astype(f32)
    cosine = rows_ref[0:1, :]
    log_sine = rows_ref[1:2, :]
    rank = lax.broadcasted_iota(jnp.int32, (1, width), 1) + 1
    log_norm = jnp.sum(jnp.where(rank <= order, rows_ref[3:4, :], 0.0), axis=1, keepdims=True)
    log_start = -0.5 * math.log(4.0 * math.pi) + log_norm + order_float * log_sine
    start = jnp.where(log_start > underflow_cut, jnp.exp(jnp.maximum(log_start, underflow_cut)), 0.0)
    degree = lax.broadcasted_iota(jnp.int32, (degrees, width), 0).astype(f32)
    raise_coef = jnp.sqrt(
        jnp.maximum(4.0 * degree * degree - 1.0, 0.0)
        / jnp.maximum(degree * degree - order_float * order_float, 1.0)
    )
    below = degree - 1.0
    lower_coef = jnp.sqrt(
        jnp.maximum(below * below - order_float * order_float, 0.0)
        / jnp.maximum(4.0 * below * below - 1.0, 1.0)
    )
    raise_ref[...] = raise_coef * cosine
    lower_ref[...] = raise_coef * lower_coef

    def advance(degree_now, carried):
        previous, earlier = carried
        row = pl.ds(degree_now, 1)
        recurred = raise_ref[row, :] * previous - lower_ref[row, :] * earlier
        current = jnp.where(degree_now == order, start, recurred)
        table_ref[row, :] = current
        return current, previous

    blank = 0.0 * raise_ref[0:1, :]
    lax.fori_loop(0, degrees, advance, (blank, blank), unroll=8)


def block_kernel(
    rings,
    depth,
    spans,
    spans_back,
    grid_hbm,
    conv_hbm,
    gain_hbm,
    mix_hbm,
    norm_hbm,
    expand_hbm,
    reduce_hbm,
    forward_hbm,
    inverse_hbm,
    rows_hbm,
    out_hbm,
    conv_ref,
    norm_ref,
    rows_ref,
    done_v,
    out_ref,
    raw_v,
    grid_v,
    halo_v,
    edge_out,
    edge_in,
    wide_v,
    first_v,
    circle_v,
    modes_v,
    column_v,
    turned_v,
    meridian_v,
    coef_own,
    coef_out,
    coef_in,
    gain_part,
    gain_all,
    gain_v,
    mix_v,
    gained_v,
    mixed_out,
    mixed_v,
    cycle_v,
    back_v,
    column_back,
    modes_all,
    spectral_own,
    spectral_out,
    spectral_in,
    normed_v,
    total_v,
    expand_v,
    reduce_v,
    forward_v,
    inverse_v,
    swap_v,
    raise_v,
    lower_v,
    table_v,
    analysis_v,
    synthesis_v,
    sems,
    local_sems,
    far_sems,
):
    sector, channels = grid_v.shape[1:]
    padded = first_v.shape[1]
    lat_count = rings * depth * 2
    swap_rows = 4 * rings
    share = mix_hbm.shape[1]
    half = coef_own.shape[0]
    lat = lax.axis_index("lat")
    lon = lax.axis_index("lon")
    x_high = rem(lat, 2)
    z = rem(div(lat, 2), depth)
    y = div(lat, 2 * depth)
    x_low = div(lon, 2)
    core = rem(lon, 2)
    plane = 4 * y + 2 * x_high + x_low
    slot = (2 * y + x_high) * 2 + core
    order = plane * depth + z
    twin = lon + 1 - 2 * core
    across = rem(lon + 2, 4)
    opposite = 3 - lon
    lat_up = rem(lat + 1, lat_count)
    lat_down = rem(lat + lat_count - 1, lat_count)
    lat_pair = lat + 1 - 2 * x_high
    lon_up = rem(lon + 1, 4)
    lon_down = rem(lon + 3, 4)
    diagonal = core == x_low

    names = {}

    def sem(name):
        index = names.setdefault(name, len(names))
        assert index < sems.shape[0], "semaphores"
        return sems.at[index]

    def send(source, target, name, lat_to, lon_to):
        copy = pltpu.make_async_remote_copy(
            src_ref=source,
            dst_ref=target,
            send_sem=sem(name + ".s"),
            recv_sem=sem(name + ".r"),
            device_id={"lat": lat_to, "lon": lon_to},
            device_id_type=MESH,
        )
        copy.start()

    def wait(ref, semaphore):
        pltpu.make_async_copy(ref, ref, semaphore).wait()

    def arrived(ref, name):
        wait(ref, sem(name + ".r"))

    def left(ref, name):
        wait(ref, sem(name + ".s"))

    def z_offset(i):
        return depth // 2 + (1 - 2 * rem(i, 2)) * div(i + 1, 2)

    def ring_peer(i):
        return rem(z + z_offset(i), depth)

    def lat_of(y_to, z_to, high_to):
        return (y_to * depth + z_to) * 2 + high_to

    def order_peer(i):
        return lat_of(div(i, 4), z, rem(div(i, 2), 2)), 2 * core + rem(i, 2)

    def cycle_peer(i):
        return lat_of(div(i, 4), z, rem(div(i, 2), 2)), 2 * rem(i, 2) + x_low

    loads = {}

    def load(name, source, target):
        copy = pltpu.make_async_copy(source, target, local_sems.at[len(loads)])
        copy.start()
        loads[name] = copy

    load("grid", grid_hbm, raw_v)
    load("rows", rows_hbm, rows_ref)
    load("conv", conv_hbm, conv_ref)
    load("norm", norm_hbm, norm_ref)
    mix_own = mix_v.at[:, pl.ds(pl.multiple_of(lon * share, 16), share), :]
    load("mix", mix_hbm, mix_own)
    load("gain0", gain_hbm.at[:, :, pl.ds(0, half)], gain_part.at[0])
    load("gain1", gain_hbm.at[:, :, pl.ds(half, half)], gain_part.at[1])
    load("forward", forward_hbm.at[core], forward_v)
    load("inverse0", inverse_hbm.at[lon], inverse_v.at[0])
    load("inverse1", inverse_hbm.at[across], inverse_v.at[1])
    load("expand", expand_hbm, expand_v)
    load("reduce", reduce_hbm, reduce_v)

    barrier = pltpu.get_barrier_semaphore()

    def greet(lat_to, lon_to):
        pl.semaphore_signal(
            barrier, inc=1, device_id={"lat": lat_to, "lon": lon_to}, device_id_type=MESH
        )

    for lat_to in (lat_up, lat_down):
        for lon_to in (lon, lon_up, lon_down):
            greet(lat_to, lon_to)
    greet(lat, lon_up)
    greet(lat, lon_down)
    greet(lat, across)
    greet(lat_pair, across)
    greet(lat_pair, opposite)

    for step in (1, depth - 1):
        greet(lat_of(y, rem(z + step, depth), x_high), lon)

    @pl.loop(0, swap_rows)
    def _(i):
        for peer in (order_peer, cycle_peer):
            lat_to, lon_to = peer(i)

            @pl.when(jnp.logical_or(lat_to != lat, lon_to != lon))
            def _():
                greet(lat_to, lon_to)

    loads["grid"].wait()
    for t in range(2):
        grid_v[t] = raw_v[:, t, :]
    blank = jnp.zeros((8 - channels // 128, 128), f32)
    for side, at in ((0, 0), (1, sector - 8)):
        pieces = []
        for t in range(2):
            line = grid_v[t, at : at + 8, :].astype(f32)[7 * side : 7 * side + 1]
            pieces += [line[:, base : base + 128] for base in range(0, channels, 128)] + [blank]
        edge_out[side] = jnp.concatenate(pieces, axis=0).astype(bf16)
    pl.semaphore_wait(barrier, 13 + 2 * swap_rows - 2 * diagonal.astype(jnp.int32))

    far_steps = [2**i for i in range(depth.bit_length()) if 2**i < depth // 2]

    def tell(i):
        for step in (far_steps[i], depth - far_steps[i]):
            pl.semaphore_signal(
                far_sems.at[i],
                inc=1,
                device_id={"lat": lat_of(y, rem(z + step, depth), x_high), "lon": lon},
                device_id_type=MESH,
            )

    def hear(i):
        pl.semaphore_wait(far_sems.at[i], 2)

    if far_steps:
        tell(0)
    for side, lon_to in ((0, lon_down), (1, lon_up)):
        for source, lat_to in ((0, lat_up), (1, lat), (2, lat_down)):
            send(edge_out.at[side], edge_in.at[side, source], "edge", lat_to, lon_to)
    def stage_halo(k):
        base, width = spans[k]
        lanes = pl.ds(base, width)
        send(grid_v.at[1, :, lanes], halo_v.at[0, :, lanes], f"halo{k}", lat_up, lon)
        send(grid_v.at[0, :, lanes], halo_v.at[1, :, lanes], f"halo{k}", lat_down, lon)

    ahead = min(halo_ahead, len(spans))
    for k in range(ahead):
        stage_halo(k)

    side = swap_rows * depth
    row = lax.broadcasted_iota(jnp.int32, (side, side), 0)
    column = lax.broadcasted_iota(jnp.int32, (side, side), 1)
    first_v[:, padded - 16 : padded, :] = jnp.zeros((2, 16, channels), bf16)
    swap_v[0] = (column == (row % depth) * swap_rows + row // depth).astype(f32).astype(bf16)
    swap_v[1] = (column == (row % swap_rows) * depth + row // swap_rows).astype(f32).astype(bf16)
    loads["rows"].wait()
    loads["conv"].wait()
    loads["norm"].wait()
    legendre_fill(order, rows_ref, raise_v, lower_v, table_v)
    table = table_v[...]
    analysis_v[...] = (table * rows_ref[2:3, :]).astype(bf16).reshape(analysis_v.shape)
    synthesis_v[...] = table.T.astype(bf16)

    for i in range(1, len(far_steps)):
        hear(i - 1)
        tell(i)

    above = (lat > 0).astype(f32)
    below = (lat < lat_count - 1).astype(f32)
    scales = (above, None, None, below)

    def edge_line(side, line, base, width):
        block = edge_in[side, (line + 1) // 2].astype(f32)
        row = 8 * (1 - line % 2) + base // 128
        return jnp.concatenate([block[i : i + 1] for i in range(row, row + width // 128)], axis=1)

    def stage_conv(k):
        base, width = spans[k]
        lanes = pl.ds(base, width)
        if k == 0:
            arrived(edge_in, "edge")
        arrived(halo_v.at[:, :, lanes], f"halo{k}")
        for line in range(4):
            source = (halo_v.at[0], grid_v.at[0], grid_v.at[1], halo_v.at[1])[line]
            body = source[:, lanes].astype(f32)
            after, before = (edge_line(side, line, base, width) for side in range(2))
            if scales[line] is not None:
                body, before, after = (scales[line] * v for v in (body, before, after))
            wide_v[line, 8 : 8 + sector, lanes] = body
            wide_v[line, 7:8, lanes] = before
            wide_v[line, 8 + sector : 9 + sector, lanes] = after
        for t in range(2):
            filtered = None
            for i in range(3):
                for j in range(3):
                    term = conv_ref[i, j : j + 1, lanes] * wide_v[t + i, 7 + j : 7 + j + sector, lanes]
                    filtered = term if filtered is None else filtered + term
            centre = wide_v[t + 1, 8 : 8 + sector, lanes]
            first_v[t, 0:sector, lanes] = (centre + jax.nn.gelu(filtered)).astype(bf16)
        send(first_v.at[1 - x_low, :, lanes], circle_v.at[lon, :, lanes], f"lonx{k}", lat, across)
        send(first_v.at[x_low, :, lanes], circle_v.at[lon, :, lanes], f"lonc{k}", lat, twin)
        circle_v[lon, :, lanes] = first_v[x_low, :, lanes]
        if k + ahead < len(spans):
            stage_halo(k + ahead)
        if k == len(spans) - 1:
            send_mix()

    def send_mix():
        loads["mix"].wait()
        rows = pl.ds(pl.multiple_of(lon * share, 16), share)
        for i, lat_to in ((0, lat_pair), (1, lat)):
            part = mix_v.at[i, rows, :]
            send(part, part, "mixx", lat_to, across)

    def send_gain():
        loads["gain0"].wait()
        loads["gain1"].wait()
        gain_all[lon] = gain_part[core]
        for i, lat_to in ((0, lat_pair), (1, lat)):
            send(gain_part.at[core, i], gain_all.at[lon, i], "gain", lat_to, across)
            send(gain_part.at[1 - core, i], gain_all.at[lon, i], "gain", lat_to, opposite)
        send(mix_own, mix_own, "mixc", lat, twin)
        send(gain_part.at[1 - core], gain_all.at[lon], "gain", lat, twin)

    def stage_relay(k):
        base, width = spans[k]
        lanes = pl.ds(base, width)
        arrived(circle_v.at[across, :, lanes], f"lonx{k}")
        send(circle_v.at[across, :, lanes], circle_v.at[across, :, lanes], f"lonr{k}", lat, twin)

    def stage_fourier(k):
        base, width = spans[k]
        lanes = pl.ds(base, width)
        if k == 0:
            loads["forward"].wait()
            if far_steps:
                hear(len(far_steps) - 1)
        arrived(circle_v.at[twin, :, lanes], f"lonc{k}")
        arrived(circle_v.at[opposite, :, lanes], f"lonr{k}")
        circle = circle_v[:, :, lanes].reshape(4 * padded, width)
        modes = jnp.dot(forward_v[...], circle, preferred_element_type=f32).astype(bf16)
        modes_v[:, :, lanes] = modes.reshape(depth, swap_rows, width)

        @pl.loop(0, depth - 1)
        def _(i):
            z_to = ring_peer(i)
            send(
                modes_v.at[z_to, :, lanes],
                column_v.at[z, :, lanes],
                f"ring{k}",
                lat_of(y, z_to, x_high),
                lon,
            )

        column_v[z, :, lanes] = modes_v[z, :, lanes]

    def stage_turn(k):
        base, width = spans[k]
        lanes = pl.ds(base, width)
        arrived(column_v.at[pl.ds(0, depth - 1), :, lanes], f"ring{k}")
        column = column_v[:, :, lanes].reshape(side, width)
        turned = jnp.dot(swap_v[0], column, preferred_element_type=f32).astype(bf16)
        turned_v[:, :, lanes] = turned.reshape(swap_rows, depth, width)

        @pl.loop(0, swap_rows)
        def _(i):
            to = rem(slot + i, swap_rows)
            lat_to, lon_to = order_peer(to)

            @pl.when(jnp.logical_or(lat_to != lat, lon_to != lon))
            def _():
                send(
                    turned_v.at[to, :, lanes],
                    meridian_v.at[plane, :, lanes],
                    f"plane{k}",
                    lat_to,
                    lon_to,
                )

        @pl.when(diagonal)
        def _():
            meridian_v[plane, :, lanes] = turned_v[slot, :, lanes]

        if k == 0:
            send_gain()

    def count_wait(ref, lanes, semaphore):
        @pl.when(diagonal)
        def _():
            wait(ref.at[pl.ds(0, swap_rows - 1), :, lanes], semaphore)

        @pl.when(jnp.logical_not(diagonal))
        def _():
            wait(ref.at[:, :, lanes], semaphore)

    def stage_analysis(k):
        base, width = spans[k]
        lanes = pl.ds(base, width)
        if k == 0:
            arrived(mix_v.at[:, pl.ds(0, share), :], "mixx")
            opposite_mix = mix_v.at[:, pl.ds(pl.multiple_of(across * share, 16), share), :]
            send(opposite_mix, opposite_mix, "mixr", lat, twin)
        count_wait(meridian_v, lanes, sem(f"plane{k}.r"))
        meridian = meridian_v[:, :, lanes].reshape(side, width)
        coef_out[:, lanes] = jnp.dot(analysis_v[1 - core], meridian, preferred_element_type=f32)
        send(coef_out.at[:, lanes], coef_in.at[:, lanes], f"coef{k}", lat, twin)
        coef_own[:, lanes] = jnp.dot(analysis_v[core], meridian, preferred_element_type=f32)

    def stage_gain(k):
        base, width = spans[k]
        lanes = pl.ds(base, width)
        if k == 0:
            arrived(gain_all.at[pl.ds(0, 3)], "gain")
            for r in range(2):
                whole = gain_all[:, r].reshape(channels, half)
                gain_v[r] = whole.T
        arrived(coef_in.at[:, lanes], f"coef{k}")
        own = coef_own[:, lanes]
        other = coef_in[:, lanes]
        real = jnp.where(core == 0, own, other)
        imag = jnp.where(core == 0, other, own)
        gain_real = gain_v[0, :, lanes]
        gain_imag = gain_v[1, :, lanes]
        gained_v[0:half, lanes] = (gain_real * real - gain_imag * imag).astype(bf16)
        gained_v[half : 2 * half, lanes] = (gain_real * imag + gain_imag * real).astype(bf16)

    def stage_mix(k):
        base, width = spans_back[k]
        lanes = pl.ds(base, width)
        if k == 0:
            arrived(mix_v.at[:, pl.ds(0, share), :], "mixc")
            arrived(mix_v.at[:, pl.ds(0, share), :], "mixr")
        gained = gained_v[...]
        contract = (((1,), (1,)), ((), ()))
        by_real = lax.dot_general(gained, mix_v[0, lanes, :], contract, preferred_element_type=f32)
        by_imag = lax.dot_general(gained, mix_v[1, lanes, :], contract, preferred_element_type=f32)
        real = by_real[:half] - by_imag[half:]
        imag = by_imag[:half] + by_real[half:]
        mixed_out[:, lanes] = jnp.where(core == 0, imag, real).astype(bf16)
        send(mixed_out.at[:, lanes], mixed_v.at[core, :, lanes], f"mixed{k}", lat, twin)
        mixed_v[core, :, lanes] = jnp.where(core == 0, real, imag).astype(bf16)

    def stage_synthesis(k):
        base, width = spans_back[k]
        lanes = pl.ds(base, width)
        arrived(mixed_v.at[1 - core, :, lanes], f"mixed{k}")
        mixed = mixed_v[:, :, lanes].reshape(2 * half, width)
        cycle = jnp.dot(synthesis_v[...], mixed, preferred_element_type=f32).astype(bf16)
        cycle_v[:, :, lanes] = cycle.reshape(swap_rows, depth, width)

        @pl.loop(0, swap_rows)
        def _(i):
            to = rem(plane + i, swap_rows)
            lat_to, lon_to = cycle_peer(to)

            @pl.when(jnp.logical_or(lat_to != lat, lon_to != lon))
            def _():
                send(
                    cycle_v.at[to, :, lanes],
                    back_v.at[slot, :, lanes],
                    f"plback{k}",
                    lat_to,
                    lon_to,
                )

        @pl.when(diagonal)
        def _():
            back_v[slot, :, lanes] = cycle_v[plane, :, lanes]

    def stage_turn_back(k):
        base, width = spans_back[k]
        lanes = pl.ds(base, width)
        count_wait(back_v, lanes, sem(f"plback{k}.r"))
        back = back_v[:, :, lanes].reshape(side, width)
        turned = jnp.dot(swap_v[1], back, preferred_element_type=f32).astype(bf16)
        column_back[:, :, lanes] = turned.reshape(depth, swap_rows, width)

        @pl.loop(0, depth - 1)
        def _(i):
            z_to = ring_peer(i)
            send(
                column_back.at[z_to, :, lanes],
                modes_all.at[core, z, :, lanes],
                f"rgback{k}",
                lat_of(y, z_to, x_high),
                lon,
            )

        modes_all[core, z, :, lanes] = column_back[z, :, lanes]

    def stage_share(k):
        base, width = spans_back[k]
        lanes = pl.ds(base, width)
        arrived(modes_all.at[core, pl.ds(0, depth - 1), :, lanes], f"rgback{k}")
        send(modes_all.at[core, :, :, lanes], modes_all.at[core, :, :, lanes], f"modes{k}", lat, twin)

    def stage_inverse(k):
        base, width = spans_back[k]
        lanes = pl.ds(base, width)
        if k == 0:
            loads["inverse0"].wait()
            loads["inverse1"].wait()
        arrived(modes_all.at[1 - core, :, :, lanes], f"modes{k}")
        modes = modes_all[:, :, :, lanes].reshape(2 * side, width)
        spectral_out[:, lanes] = jnp.dot(
            inverse_v[1], modes, preferred_element_type=f32
        ).astype(bf16)
        send(spectral_out.at[:, lanes], spectral_in.at[:, lanes], f"spec{k}", lat, across)
        spectral_own[:, lanes] = jnp.dot(inverse_v[0], modes, preferred_element_type=f32)

    def finish(which, spectral):
        second = (first_v[which].astype(f32) + spectral).astype(bf16).astype(f32)
        scale = lax.rsqrt(jnp.mean(second * second, axis=-1, keepdims=True) + norm_eps)
        normed_v[...] = (second * norm_ref[...].reshape(1, channels) * scale).astype(bf16)
        total_v[...] = second
        hidden_width = expand_v.shape[1]
        step = min(256, hidden_width)
        for base in range(0, hidden_width, step):
            columns = slice(base, base + step)
            hidden = jax.nn.gelu(
                jnp.dot(normed_v[...], expand_v[:, columns], preferred_element_type=f32)
            ).astype(bf16)
            total_v[...] += jnp.dot(hidden, reduce_v[columns, :], preferred_element_type=f32)
        done_v[which] = total_v[...].astype(bf16)

    def run(count, stages, lags):
        for beat in range(count + max(lags)):
            for stage, lag in reversed(list(zip(stages, lags))):
                if 0 <= beat - lag < count:
                    stage(beat - lag)

    count = len(spans)
    run(count, [stage_conv, stage_relay, stage_fourier], front_lags)
    run(count, [stage_turn, stage_analysis, stage_gain], middle_lags)
    count = len(spans_back)
    late = [stage_mix, stage_synthesis, stage_turn_back, stage_share, stage_inverse]
    run(count, late, [0, count, 2 * count, 3 * count, 3 * count + 1])

    loads["expand"].wait()
    loads["reduce"].wait()
    finish(x_low, spectral_own[...])
    for k, (base, width) in enumerate(spans_back):
        arrived(spectral_in.at[:, pl.ds(base, width)], f"spec{k}")
    finish(1 - x_low, spectral_in[...].astype(f32))

    for t in range(2):
        out_ref[:, t, :] = done_v[t, 0:sector, :]
    load("out", out_ref, out_hbm)
    loads["out"].wait()
    left(edge_in, "edge")
    left(mix_v.at[:, pl.ds(0, share), :], "mixx")
    left(mix_v.at[:, pl.ds(0, share), :], "mixc")
    left(mix_v.at[:, pl.ds(0, share), :], "mixr")
    left(gain_all.at[pl.ds(0, 3)], "gain")
    for k, (base, width) in enumerate(spans):
        lanes = pl.ds(base, width)
        left(halo_v.at[:, :, lanes], f"halo{k}")
        for name in ("lonx", "lonc", "lonr"):
            left(circle_v.at[0, :, lanes], f"{name}{k}")
        left(column_v.at[pl.ds(0, depth - 1), :, lanes], f"ring{k}")
        count_wait(meridian_v, lanes, sem(f"plane{k}.s"))
        left(coef_in.at[:, lanes], f"coef{k}")
    for k, (base, width) in enumerate(spans_back):
        lanes = pl.ds(base, width)
        left(mixed_out.at[:, lanes], f"mixed{k}")
        count_wait(back_v, lanes, sem(f"plback{k}.s"))
        left(column_v.at[pl.ds(0, depth - 1), :, lanes], f"rgback{k}")
        left(modes_all.at[0, :, :, lanes], f"modes{k}")
        left(spectral_out.at[:, lanes], f"spec{k}")


def spans_of(tiles):
    edges = np.concatenate([[0], np.cumsum(tiles)]) * 128
    return [(int(a), int(b - a)) for a, b in zip(edges, edges[1:])]


front_tiles = (1, 2, 2)
back_tiles = (2, 2, 1)
halo_ahead = 2
front_lags = (0, 1, 2)
middle_lags = (0, 3, 6)


def shards(
    rings,
    depth,
    grid_state,
    conv_weight,
    spectral_gain,
    spectral_weight,
    norm_gain,
    expand_weight,
    reduce_weight,
):
    two, sector, channels = grid_state.shape
    padded = -(-sector // 16) * 16
    degrees = spectral_gain.shape[1]
    lat_total = 4 * rings * depth
    side = lat_total
    swap_rows = 4 * rings
    half = degrees // 2
    share = channels // 4
    hidden_width = expand_weight.shape[1]
    spans, spans_back = spans_of(front_tiles), spans_of(back_tiles)
    forward, inverse = fourier_tables(sector, padded, degrees, rings, depth)
    rows = jnp.asarray(latitude_rows(lat_total, rings, depth))
    anywhere = pl.BlockSpec(memory_space=pl.ANY)
    scratch = [
        (conv_weight.shape, f32),
        (norm_gain.shape, f32),
        (rows.shape, f32),
        ((2, padded, channels), bf16),
        ((sector, 2, channels), bf16),
        ((sector, 2, channels), bf16),
        ((2, sector, channels), bf16),
        ((2, sector, channels), bf16),
        ((2, edge_rows, 128), bf16),
        ((2, 3, edge_rows, 128), bf16),
        ((4, -(-(sector + 16) // 8) * 8, channels), f32),
        ((2, padded, channels), bf16),
        ((4, padded, channels), bf16),
        ((depth, swap_rows, channels), bf16),
        ((depth, swap_rows, channels), bf16),
        ((swap_rows, depth, channels), bf16),
        ((swap_rows, depth, channels), bf16),
        ((half, channels), f32),
        ((half, channels), f32),
        ((half, channels), f32),
        ((2, 2, share, half), f32),
        ((4, 2, share, half), f32),
        ((2, half, channels), f32),
        ((2, channels, channels), bf16),
        ((2 * half, channels), bf16),
        ((half, channels), bf16),
        ((2, half, channels), bf16),
        ((swap_rows, depth, channels), bf16),
        ((swap_rows, depth, channels), bf16),
        ((depth, swap_rows, channels), bf16),
        ((2, depth, swap_rows, channels), bf16),
        ((padded, channels), f32),
        ((padded, channels), bf16),
        ((padded, channels), bf16),
        ((padded, channels), bf16),
        ((padded, channels), f32),
        ((channels, hidden_width), bf16),
        ((hidden_width, channels), bf16),
        ((side, 4 * padded), bf16),
        ((2, padded, 2 * side), bf16),
        ((2, side, side), bf16),
        ((degrees, lat_total), f32),
        ((degrees, lat_total), f32),
        ((degrees, lat_total), f32),
        ((2, half, lat_total), bf16),
        ((lat_total, degrees), bf16),
    ]
    block_output = pl.pallas_call(
        functools.partial(block_kernel, rings, depth, spans, spans_back),
        out_shape=jax.ShapeDtypeStruct((sector, 2, channels), bf16),
        in_specs=[anywhere] * 10,
        out_specs=anywhere,
        scratch_shapes=[pltpu.VMEM(*s) for s in scratch]
        + [
            pltpu.SemaphoreType.DMA((10 + 14 * len(spans) + 10 * len(spans_back),)),
            pltpu.SemaphoreType.DMA((14,)),
            pltpu.SemaphoreType.REGULAR((max(1, depth.bit_length()),)),
        ],
        compiler_params=pltpu.CompilerParams(
            collective_id=0, has_side_effects=True, vmem_limit_bytes=60 * 1024 * 1024
        ),
        name="block_pair",
    )(
        jnp.swapaxes(grid_state, 0, 1),
        conv_weight,
        jnp.swapaxes(spectral_gain, 1, 2),
        jnp.swapaxes(spectral_weight, 1, 2),
        norm_gain,
        expand_weight,
        reduce_weight,
        forward,
        inverse,
        rows,
    )
    return jnp.swapaxes(block_output, 0, 1)


def solution(mesh):
    lat_count = mesh.shape["lat"]
    rings = max(1, lat_count // 32)
    depth = lat_count // (2 * rings)
    return jax.shard_map(
        functools.partial(shards, rings, depth),
        mesh=mesh,
        in_specs=(
            P("lat", "lon", None),
            P(),
            P(None, None, "lon"),
            P(None, None, "lon"),
            P(),
            P(),
            P(),
        ),
        out_specs=P("lat", "lon", None),
        check_vma=False,
    )
```
